128 devices in a mesh: lat: 64 (over z, x, y), head: 2 (over core).
Axes of the slice: x: 4, y: 4, z: 4, core: 2. Of those that a mesh axis runs over, the one named last changes fastest.
Arguments:
- grid_latent: bfloat16 [524288, 512], P('lat'), may hold values from -6 to 6
- mesh_latent: bfloat16 [40960, 512], P('lat'), may hold values from -6 to 6
- neighbours: int32 [40960, 16], P('lat'), may hold values from -1 to 524287, as said below
- edge_bias: bfloat16 [40960, 64], P('lat', 'head'), may hold values from -8 to 384
- query_weight: bfloat16 [512, 512], P(None, 'head'), may hold values from -0.25 to 0.25
- key_weight: bfloat16 [512, 512], P(None, 'head'), may hold values from -0.25 to 0.25
- value_weight: bfloat16 [512, 512], P(None, 'head'), may hold values from -0.25 to 0.25
- out_weight: bfloat16 [512, 512], P('head'), may hold values from -0.25 to 0.25
- norm_gain: bfloat16 [512], P('head'), may hold values from 0.5 to 1.5
Outputs:
- mesh_out: bfloat16 [40960, 512], P('lat', 'head')
The draws below stay inside these ranges and needn't reach their ends.
Inputs may be any that keep to these rules, and one draw needn't show every extreme that they name: `neighbours`: every neighbour of mesh node m is -1 or lies in [b * 8192 - 2048, (b + 1) * 8192 + 2048) with b = m // 640; both ends of that range (cut to the grid) are named in every draw; slots 0 and 1 are never -1.
All inputs are finite; a program needn't handle non-finite values.
Results may differ from the reference program's by a relative error of at most 0.0075.
Values may be sent and summed in bfloat16 or wider, within the bound.
A program may use at most 128 MiB of HBM per device.

```python
import math
import jax
import jax.numpy as jnp
from jax import lax

D = 512
HEADS = 4
K = 16
G_DEV = 8192
M_DEV = 640
HEAD_DIM = 128
HALO = 2048
GRID = 524288
MESH = 40960


def draw_neighbours(key, part):
    mesh_ids = jnp.arange(MESH, dtype=jnp.int32)
    owner = mesh_ids // M_DEV
    lowest = jnp.maximum(owner * G_DEV - HALO, 0)
    highest = jnp.minimum((owner + 1) * G_DEV + HALO, GRID)
    key_pick = jax.random.fold_in(key, 11)
    key_pad = jax.random.fold_in(key, 23)
    offsets = jax.random.randint(key_pick, (MESH, K), 0, (highest - lowest)[:, None])
    picked = lowest[:, None] + offsets
    first = (mesh_ids % M_DEV == 0)[:, None]
    slot = jnp.arange(K, dtype=jnp.int32)[None, :]
    picked = jnp.where(first & (slot == 0), lowest[:, None], picked)
    picked = jnp.where(first & (slot == 1), highest[:, None] - 1, picked)
    padded = (jax.random.randint(key_pad, (MESH, K), 0, 4) == 0) & (slot >= 2)
    return jnp.where(padded, -1, picked).astype(jnp.int32)


def draw_edge_bias(key, part):
    base = jnp.clip(jax.random.normal(jax.random.fold_in(key, 37), (MESH, HEADS * K), jnp.float32), -8.0, 8.0)
    return base.astype(jnp.bfloat16)


def shard_levels(key, extent, cuts, smallest, high):
    def one(dim, shards_of):
        steps = jax.random.uniform(jax.random.fold_in(jax.random.fold_in(key, 6), dim), (shards_of,), jnp.float32, smallest / len(cuts), high / len(cuts))
        return jnp.repeat(jnp.exp(steps), extent[dim] // shards_of).reshape((-1,) + (1,) * (len(extent) - dim - 1))

    level = one(*cuts[0])
    for cut in cuts[1:]:
        level = level * one(*cut)
    return level


def gaussian(key, dims, deviation, limit, shards=(), kind=jnp.bfloat16):
    array = jax.random.normal(key, dims, jnp.float32) * deviation
    if len(shards) > 0:
        array = shard_levels(key, dims, shards, -0.22, 0.18) * array
    return jnp.clip(array, min=-limit, max=limit).astype(kind)


def setup_inputs(seed: int = 0) -> dict:
    splits = jax.random.split(jax.random.key(seed), 10)
    grid_latent = gaussian(splits[0], (GRID, D), 1.0, 6.0, ((0, 64),))
    mesh_latent = gaussian(splits[1], (MESH, D), 1.0, 6.0, ((0, 64),))
    neighbours = draw_neighbours(jax.random.fold_in(splits[9], 71), 0)
    edge_bias = draw_edge_bias(jax.random.fold_in(splits[9], 71), 0)
    query_weight = gaussian(splits[4], (D, D), D ** -0.5, 0.25, ((1, 2),))
    key_weight = gaussian(splits[5], (D, D), D ** -0.5, 0.25, ((1, 2),))
    value_weight = gaussian(splits[6], (D, D), D ** -0.5, 0.25, ((1, 2),))
    out_weight = gaussian(splits[7], (D, D), D ** -0.5, 0.25, ((0, 2),))
    norm_gain = jnp.clip(1.0 + 0.1 * jax.random.normal(splits[8], (D,), jnp.float32), 0.5, 1.5).astype(jnp.bfloat16)
    return dict(grid_latent=grid_latent, mesh_latent=mesh_latent, neighbours=neighbours, edge_bias=edge_bias, query_weight=query_weight, key_weight=key_weight, value_weight=value_weight, out_weight=out_weight, norm_gain=norm_gain)


EPSILON = 1e-05

def reference(grid_latent, mesh_latent, neighbours, edge_bias, query_weight, key_weight, value_weight, out_weight, norm_gain):

    def attend_block(blocks):
        mesh_rows, neigh_rows, bias_rows = blocks
        count = mesh_rows.shape[0]
        queries = jnp.dot(mesh_rows, query_weight, preferred_element_type=jnp.float32).astype(jnp.bfloat16)
        valid = neigh_rows >= 0
        safe_index = jnp.where(valid, neigh_rows, 0).astype(jnp.int32)
        fetched = grid_latent[safe_index.reshape(-1)]
        keys = jnp.dot(fetched, key_weight, preferred_element_type=jnp.float32).astype(jnp.bfloat16)
        values = jnp.dot(fetched, value_weight, preferred_element_type=jnp.float32).astype(jnp.bfloat16)
        keys = keys.reshape(count, K, HEADS, HEAD_DIM).astype(jnp.float32)
        values = values.reshape(count, K, HEADS, HEAD_DIM).astype(jnp.float32)
        query_heads = queries.astype(jnp.float32).reshape(count, HEADS, HEAD_DIM)
        scores = jnp.einsum('bhc,bkhc->bhk', query_heads, keys) * HEAD_DIM ** (-0.5)
        scores = scores + bias_rows.astype(jnp.float32).reshape(count, HEADS, K)
        live = valid[:, None, :]
        scores = jnp.where(live, scores, -1e+30)
        top_score = lax.optimization_barrier(jnp.max(scores, axis=2, keepdims=True))
        weights = jnp.where(live, jnp.exp(scores - top_score), 0.0)
        total = lax.optimization_barrier(jnp.sum(weights, axis=2))
        mixed = jnp.einsum('bhk,bkhc->bhc', weights, values) / total[:, :, None]
        attended = mixed.reshape(count, D).astype(jnp.bfloat16)
        projected = jnp.dot(attended, out_weight, preferred_element_type=jnp.float32)
        updated = mesh_rows.astype(jnp.float32) + projected
        mean = lax.optimization_barrier(jnp.sum(updated, axis=1)) / D
        variance = lax.optimization_barrier(jnp.sum(updated * updated, axis=1)) / D - mean * mean
        normed = (updated - mean[:, None]) * lax.rsqrt(variance[:, None] + EPSILON) * norm_gain.astype(jnp.float32)
        return normed.astype(jnp.bfloat16)
    block = math.gcd(MESH, 512)
    nblocks = MESH // block
    result = lax.map(attend_block, (mesh_latent.reshape(nblocks, block, D), neighbours.reshape(nblocks, block, K), edge_bias.reshape(nblocks, block, HEADS * K)))
    return result.reshape(MESH, D)
```

```python
import functools

import jax
import jax.numpy as jnp
from jax import lax
from jax.experimental import pallas as pl
from jax.experimental.pallas import tpu as pltpu
from jax.sharding import PartitionSpec as P

D = 512
K = 16
HEADS = 4
HEAD_DIM = 128
HALO = 2048
EPSILON = 1e-05
TN = 32
CH = 512
DEAD = -1e30
VMEM = pl.BlockSpec(memory_space=pltpu.VMEM)
SMEM = pl.BlockSpec(memory_space=pltpu.SMEM)
ANY = pl.BlockSpec(memory_space=pl.ANY)
NT = (((1,), (1,)), ((), ()))
F32 = jnp.float32
BF16 = jnp.bfloat16


def compact_kernel(nb_ref, bias_ref, idx_ref, same_ref, cross_ref, *, band):
    first = lax.axis_index("head") == 0
    offset = lax.axis_index("lat") * band
    local = [nb_ref[k] - offset for k in range(K)]
    live = [nb_ref[k] >= 0 for k in range(K)]
    up = [local[k] >= band for k in range(K)]
    down = [live[k] & (local[k] < 0) for k in range(K)]
    for same in (True, False):
        use_up = first if same else jnp.logical_not(first)
        rank = []
        count = jnp.zeros(local[0].shape, jnp.int32)
        for k in range(K):
            here = jnp.where(use_up, up[k].astype(jnp.int32), down[k].astype(jnp.int32))
            rank.append(jnp.where(here > 0, count, -1))
            count = count + here
        shift = jnp.where(use_up, -band, HALO)
        out = same_ref if same else cross_ref
        for r in range(K):
            row = jnp.zeros(local[0].shape, jnp.int32)
            biases = [jnp.full(local[0].shape, DEAD, F32) for _ in range(2)]
            for k in range(r, K):
                hit = rank[k] == r
                if same:
                    row = jnp.where(hit, (local[k] + shift) * 4, row)
                for h in range(2):
                    biases[h] = jnp.where(hit, bias_ref[h * K + k], biases[h])
            if same:
                idx_ref[r] = row
            for h in range(2):
                out[h * K + r] = biases[h]


def compact(nb, bias, band):
    shape = nb.shape
    return pl.pallas_call(
        functools.partial(compact_kernel, band=band),
        out_shape=(
            jax.ShapeDtypeStruct(shape, jnp.int32),
            jax.ShapeDtypeStruct((2 * K,) + shape[1:], F32),
            jax.ShapeDtypeStruct((2 * K,) + shape[1:], F32),
        ),
        in_specs=[VMEM] * 2,
        out_specs=(VMEM,) * 3,
    )(nb, bias)


def attend_kernel(
    tiles, slots, rows, side, grid_ref, idx_ref, over_ref, bias_ref, mesh_ref, w_ref, v_ref, att_ref, lse_ref,
    buf, sems, table, st0, st1, qs, cs, gs, ss,
):
    edges = slots * TN
    base = lax.axis_index("head") * side
    chunks = rows // CH
    copies = [
        pltpu.make_async_copy(
            grid_ref.at[pl.ds(pl.multiple_of(base + i * CH, CH), CH), :], buf.at[pl.ds(i * CH, CH), :], sems.at[i]
        )
        for i in range(chunks)
    ]
    for copy in copies:
        copy.start()
    for pair in range(2):
        wq = w_ref[pair, :, 0:256]
        wk = w_ref[pair, :, 256:512]
        q = jnp.dot(mesh_ref[...], wq, preferred_element_type=F32).astype(BF16)
        for j in range(2):
            s = slice(j * HEAD_DIM, (j + 1) * HEAD_DIM)
            qk = lax.dot_general(q[:, s], wk[:, s], NT, preferred_element_type=F32)
            qs[2 * pair + j] = (qk * HEAD_DIM ** -0.5).astype(BF16)
    for i in range(chunks):
        copies[i].wait()
        for c in range(4):
            table[pl.ds(i * CH * 4 + c, CH, stride=4), :] = buf[pl.ds(i * CH, CH), c * 128:(c + 1) * 128].astype(F32)

    def same(width):
        node = lax.broadcasted_iota(jnp.int32, (TN, width), 0)
        lane = lax.broadcasted_iota(jnp.int32, (TN, width), 1)
        return (lane % TN) == node

    def gather(t, st, count):
        for p in range(count):
            st[pl.ds(4 * p, 4), :] = table[pl.ds(pl.multiple_of(idx_ref[t * (K * TN) + p], 4), 4), :]

    def staged(st, count):
        return jnp.concatenate([st[pl.ds(c, count, stride=4), :].astype(BF16) for c in range(4)], axis=1)

    def scores(t, g):
        r0 = pl.multiple_of(t * TN, TN)
        qt = jnp.concatenate([qs[h, pl.ds(r0, TN), :] for h in range(HEADS)], axis=0)
        sc = lax.dot_general(qt, g, NT, preferred_element_type=F32)
        mask = same(g.shape[0])
        return jnp.concatenate(
            [jnp.sum(jnp.where(mask, sc[h * TN:(h + 1) * TN], 0.0), axis=0, keepdims=True) for h in range(HEADS)], axis=0
        )

    def softmax(s):
        width = s.shape[1]

        def fold(x, op):
            y = x[:, 0:128]
            for j in range(1, width // 128):
                y = op(y, x[:, j * 128:(j + 1) * 128])
            y = op(y, pltpu.roll(y, 64, 1))
            return op(y, pltpu.roll(y, 32, 1))

        m = fold(s, jnp.maximum)
        w = jnp.exp(s - jnp.concatenate([m] * (width // 128), axis=1))
        total = fold(w, jnp.add)
        w = w * jnp.concatenate([1.0 / total] * (width // 128), axis=1)
        return w, m + jnp.log(total)

    def mix(t, w, g):
        mask = same(g.shape[0])
        pt = jnp.concatenate([jnp.where(mask, w[h:h + 1], 0.0).astype(BF16) for h in range(HEADS)], axis=0)
        ctx = jnp.dot(pt, g, preferred_element_type=F32)
        r0 = pl.multiple_of(t * TN, TN)
        for h in range(HEADS):
            cs[h, pl.ds(r0, TN), :] = ctx[h * TN:(h + 1) * TN].astype(BF16)

    gather(0, st0, edges)

    @pl.loop(0, tiles // 2)
    def _(i):
        t = 2 * i
        gather(t + 1, st1, edges)
        g0 = staged(st0, edges)
        s0 = scores(t, g0)
        gs[pl.ds(pl.multiple_of(t * edges, edges), edges), :] = g0
        gather(jnp.minimum(t + 2, tiles - 1), st0, edges)
        g1 = staged(st1, edges)
        s1 = scores(t + 1, g1)
        gs[pl.ds(pl.multiple_of((t + 1) * edges, edges), edges), :] = g1
        r0 = pl.multiple_of(i * 8, 8)
        ss[pl.ds(r0, 8), 0:edges] = jnp.concatenate([s0, s1], axis=0)

    w, lse = softmax(ss[:, 0:edges] + bias_ref[:, 0:edges])
    ss[:, 0:edges] = w
    lse_ref[...] = lse

    @pl.loop(0, tiles // 2)
    def _(i):
        both = ss[pl.ds(pl.multiple_of(i * 8, 8), 8), 0:edges]
        for j in range(2):
            t = 2 * i + j
            mix(t, both[4 * j:4 * j + 4], gs[pl.ds(pl.multiple_of(t * edges, edges), edges), :])

    if slots < K:

        def again(i, j):
            t = 2 * i + j
            full = K * TN
            gather(t, st0, full)
            g = staged(st0, full)
            rows8 = pl.ds(pl.multiple_of(i * 8, 8), 8)
            w, lse = softmax(scores(t, g) + bias_ref[rows8, :][4 * j:4 * j + 4])
            old = lse_ref[rows8, :]
            lse_ref[rows8, :] = jnp.concatenate([old[0:4], lse] if j else [lse, old[4:8]], axis=0)
            mix(t, w, g)

        @pl.loop(0, tiles // 2)
        def _(i):
            for j in range(2):
                pl.when(over_ref[2 * i + j] > 0)(functools.partial(again, i, j))

    for h in range(HEADS):
        s = slice(h * HEAD_DIM, (h + 1) * HEAD_DIM)
        wv = v_ref[h // 2, :, (h % 2) * HEAD_DIM:(h % 2 + 1) * HEAD_DIM]
        att_ref[:, s] = jnp.dot(cs[h], wv, preferred_element_type=F32).astype(BF16)


def attend(grid, idx, over, bias, mesh, w, v, *, slots, rows, side):
    nodes = mesh.shape[0]
    tiles = nodes // TN
    edges = slots * TN
    return pl.pallas_call(
        functools.partial(attend_kernel, tiles, slots, rows, side),
        out_shape=(jax.ShapeDtypeStruct((nodes, D), BF16), jax.ShapeDtypeStruct((tiles * HEADS, 128), F32)),
        in_specs=[ANY, SMEM, SMEM, VMEM, VMEM, VMEM, VMEM],
        out_specs=(VMEM, VMEM),
        scratch_shapes=[
            pltpu.VMEM((rows, D), BF16),
            pltpu.SemaphoreType.DMA((rows // CH,)),
            pltpu.VMEM((rows * 4, 128), F32),
            pltpu.VMEM((K * TN * 4, 128), F32),
            pltpu.VMEM((edges * 4, 128), F32),
            pltpu.VMEM((HEADS, nodes, D), BF16),
            pltpu.VMEM((HEADS, nodes, D), BF16),
            pltpu.VMEM((tiles * edges, D), BF16),
            pltpu.VMEM((tiles * HEADS, K * TN), F32),
        ],
        compiler_params=pltpu.CompilerParams(vmem_limit_bytes=56 * 1024 * 1024),
    )(grid, idx, over, bias, mesh, w, v)


def final_kernel(a0, a1, a2, l0, l1, l2, mesh_ref, wo_ref, gain_ref, keep_ref, send_ref, *, last):
    first = lax.axis_index("head") == 0
    lat = lax.axis_index("lat")
    has_low, has_high = lat > 0, lat < last
    has1 = jnp.where(first, has_high, has_low)
    has2 = jnp.where(first, has_low, has_high)
    nodes = mesh_ref.shape[0]
    tiles = nodes // TN
    x0 = l0[...]
    x1 = jnp.where(has1, l1[...], DEAD)
    rows = 4 * tiles
    order = lax.broadcasted_iota(jnp.int32, (rows, 128), 0) % 4
    swapped = jnp.where(order < 2, pltpu.roll(l2[...], rows - 2, 0), pltpu.roll(l2[...], 2, 0))
    x2 = jnp.where(has2, swapped, DEAD)
    top = jnp.maximum(x0, jnp.maximum(x1, x2))
    e = [jnp.exp(x - top) for x in (x0, x1, x2)]
    inv = 1.0 / (e[0] + e[1] + e[2])
    e = [x * inv for x in e]
    node = lax.broadcasted_iota(jnp.int32, (TN, 128), 0)
    lane = lax.broadcasted_iota(jnp.int32, (TN, 128), 1)
    mask = node == lane

    def column(i, h):
        parts = [
            jnp.sum(jnp.where(mask, e[i][t * 4 + h:t * 4 + h + 1, :], 0.0), axis=1, keepdims=True) for t in range(tiles)
        ]
        return jnp.concatenate(parts, axis=0)

    heads = []
    for h in range(HEADS):
        s = slice(h * HEAD_DIM, (h + 1) * HEAD_DIM)
        hx = (h + 2) % 4
        sx = slice(hx * HEAD_DIM, (hx + 1) * HEAD_DIM)
        mixed = (
            a0[:, s].astype(F32) * column(0, h)
            + a1[:, s].astype(F32) * column(1, h)
            + a2[:, sx].astype(F32) * column(2, h)
        )
        heads.append(mixed.astype(BF16))
    mine = jnp.concatenate(heads[0:2], axis=1)
    theirs = jnp.concatenate(heads[2:4], axis=1)
    projected = jnp.dot(mine, wo_ref[0], preferred_element_type=F32) + jnp.dot(
        theirs, wo_ref[1], preferred_element_type=F32
    )
    updated = mesh_ref[...].astype(F32) + projected
    mean = jnp.sum(updated, axis=1, keepdims=True) / D
    variance = jnp.sum(updated * updated, axis=1, keepdims=True) / D - mean * mean
    normed = (updated - mean) * lax.rsqrt(variance + EPSILON)
    left, right = normed[:, 0:256], normed[:, 256:512]
    keep_ref[...] = (jnp.where(first, left, right) * gain_ref[0:1, :]).astype(BF16)
    send_ref[...] = (jnp.where(first, right, left) * gain_ref[1:2, :]).astype(BF16)


def finish(own, r0, r1, mesh, wo, gain, last):
    nodes = mesh.shape[0]
    return pl.pallas_call(
        functools.partial(final_kernel, last=last),
        out_shape=(jax.ShapeDtypeStruct((nodes, D // 2), BF16),) * 2,
        in_specs=[VMEM] * 9,
        out_specs=(VMEM, VMEM),
    )(own[0], r0[0], r1[0], own[1], r0[1], r1[1], mesh, wo, gain)


def shards(
    grid_latent, mesh_latent, neighbours, edge_bias, query_weight, key_weight, value_weight, out_weight, norm_gain
):
    band = grid_latent.shape[0]
    count = mesh_latent.shape[0]
    half = count // 2
    lats = lax.axis_size("lat")
    c = lax.axis_index("head")
    offset = lax.axis_index("lat") * band
    both = ("lat", "head")

    def partner(x):
        return lax.ppermute(x, "head", [(0, 1), (1, 0)])

    def outward(cross):
        pairs = []
        for b in range(lats):
            if b + 1 < lats:
                pairs.append((2 * b + (1 if cross else 0), 2 * (b + 1)))
            if b > 0:
                pairs.append((2 * b + (0 if cross else 1), 2 * (b - 1) + 1))
        return pairs

    def homeward(cross):
        return [(target, source ^ (1 if cross else 0)) for source, target in outward(False)]

    def mine_of(x):
        return lax.dynamic_slice_in_dim(x, c * half, half, 0)

    def other_of(x):
        return lax.dynamic_slice_in_dim(x, (1 - c) * half, half, 0)

    mesh_c, mesh_o = mine_of(mesh_latent), other_of(mesh_latent)
    qa = lax.ppermute(mesh_c, both, outward(False))
    weights = jnp.concatenate([query_weight, key_weight], axis=1)
    weights = jnp.stack([weights, partner(weights)])
    values = jnp.stack([value_weight, partner(value_weight)])
    bias_o = partner(other_of(edge_bias))
    qb = lax.ppermute(mesh_o, both, outward(False))
    outs = jnp.stack([out_weight, partner(out_weight)])

    lanes = (count // 128, 128)
    nb_t = neighbours.T.reshape((K,) + lanes)
    bias_t = edge_bias.astype(F32).T.reshape((2 * K,) + lanes)
    idx, bias_same, bias_cross = compact(nb_t, bias_t, band)
    idx = lax.ppermute(idx, both, outward(False))
    bias_same = lax.ppermute(bias_same.astype(BF16), both, outward(False))
    bias_cross = lax.ppermute(bias_cross.astype(BF16), both, outward(True))

    tiles = half // TN
    nb_c = mine_of(neighbours) - offset
    inside = (nb_c >= 0) & (nb_c < band) & (mine_of(neighbours) >= 0)

    def tiled(x):
        return x.reshape(tiles, TN, K).transpose(0, 2, 1)

    own_idx = tiled(jnp.where(inside, nb_c * 4, 0)).reshape(-1)
    own_bias = jnp.concatenate([mine_of(edge_bias), bias_o], axis=1).astype(F32)
    own_bias = own_bias.reshape(tiles, TN, HEADS, K).transpose(0, 2, 3, 1)
    own_bias = jnp.where(tiled(inside)[:, None], own_bias, DEAD).reshape(tiles * HEADS, K * TN)
    none = jnp.zeros((tiles,), jnp.int32)
    own = attend(grid_latent, own_idx, none, own_bias, mesh_c, weights, values, slots=K, rows=band, side=0)

    idx = idx.reshape(K, 2 * tiles, TN).transpose(1, 0, 2)
    bias = jnp.concatenate([bias_same, bias_cross], axis=0).astype(F32).reshape(HEADS, K, 2 * tiles, TN)
    over = jnp.max(bias[0, 8], axis=1) > DEAD / 2
    bias = bias.transpose(2, 0, 1, 3)
    over = over.astype(jnp.int32)

    def visit(mesh, pick):
        return attend(
            grid_latent,
            pick(idx).reshape(-1),
            pick(over),
            pick(bias).reshape(tiles * HEADS, K * TN),
            mesh,
            weights,
            values,
            slots=8,
            rows=HALO,
            side=band - HALO,
        )

    def pick_mine(x):
        return lax.dynamic_slice_in_dim(x, c * tiles, tiles, 0)

    def pick_other(x):
        return lax.dynamic_slice_in_dim(x, (1 - c) * tiles, tiles, 0)

    na = visit(qa, pick_mine)
    r0 = [lax.ppermute(x, both, homeward(False)) for x in na]
    nb = visit(qb, pick_other)
    r1 = [lax.ppermute(x, both, homeward(True)) for x in nb]
    gain = norm_gain.astype(F32)[None]
    gain = jnp.concatenate([gain, partner(gain)], axis=0)
    keep, send = finish(own, r0, r1, mesh_c, outs, gain, lats - 1)
    got = partner(send)
    return jnp.where(c == 0, jnp.concatenate([keep, got], axis=0), jnp.concatenate([got, keep], axis=0))


def solution(mesh):
    in_specs = (
        P("lat", None),
        P("lat", None),
        P("lat", None),
        P("lat", "head"),
        P(None, "head"),
        P(None, "head"),
        P(None, "head"),
        P("head", None),
        P("head"),
    )
    out_specs = P("lat", "head")
    return jax.shard_map(shards, mesh=mesh, in_specs=in_specs, out_specs=out_specs, check_vma=False)
```

```python
import functools

import jax
import jax.numpy as jnp
from jax import lax
from jax.experimental import pallas as pl
from jax.experimental.pallas import tpu as pltpu
from jax.sharding import PartitionSpec as P

D = 512
K = 16
HEADS = 4
HEAD_DIM = 128
HALO = 2048
EPSILON = 1e-05
TN = 32
EDGES = K * TN
CH = 512
PIECE = 256
DEAD = -1e30
VMEM = pl.BlockSpec(memory_space=pltpu.VMEM)
SMEM = pl.BlockSpec(memory_space=pltpu.SMEM)
ANY = pl.BlockSpec(memory_space=pl.ANY)
MESH = pl.DeviceIdType.MESH
NT = (((1,), (1,)), ((), ()))
F32 = jnp.float32
BF16 = jnp.bfloat16


def kernel(
    last, grid_ref, idx_ref, bias_ref, mesh_ref, wq_ref, wk_ref, wv_ref, wo_ref, gain_ref, out_ref,
    buf, hbuf, table, st0, st1, qs, cs, gs, ss, wq2, wk2, wv2, wo2, gain2, bias2, out_send, out_recv,
    load_sem, ici_send, ici_recv, fwd_send, fwd_recv, w_send, w_recv, x_send, x_recv,
):
    band = grid_ref.shape[0]
    half = mesh_ref.shape[0] // 2
    tiles = half // TN
    share = HALO // 2
    pieces = share // PIECE
    lat = lax.axis_index("lat")
    c = lax.axis_index("head")
    other = 1 - c
    has_low, has_high = lat > 0, lat < last
    below, above = jnp.maximum(lat - 1, 0), jnp.minimum(lat + 1, last)

    chunks = band // CH
    loads = [
        pltpu.make_async_copy(grid_ref.at[pl.ds(i * CH, CH), :], buf.at[pl.ds(i * CH, CH), :], load_sem.at[i])
        for i in range(chunks)
    ]
    for load in loads:
        load.start()

    barrier = pltpu.get_barrier_semaphore()
    pl.semaphore_signal(barrier, inc=1, device_id=(lat, other), device_id_type=MESH)

    @pl.when(has_low)
    def _():
        pl.semaphore_signal(barrier, inc=1, device_id=(below, c), device_id_type=MESH)

    @pl.when(has_high)
    def _():
        pl.semaphore_signal(barrier, inc=1, device_id=(above, c), device_id_type=MESH)

    pl.semaphore_wait(barrier, 1 + has_low.astype(jnp.int32) + has_high.astype(jnp.int32))

    def crossing(side, i):
        start = band - HALO if side == 0 else 0
        rows = pl.ds(pl.multiple_of(start + c * share + i * PIECE, PIECE), PIECE)
        return pltpu.make_async_remote_copy(
            src_ref=grid_ref.at[rows, :],
            dst_ref=hbuf.at[side, 0, pl.ds(i * PIECE, PIECE), :],
            send_sem=ici_send.at[side, i],
            recv_sem=ici_recv.at[side, i],
            device_id=(above if side == 0 else below, c),
            device_id_type=MESH,
        )

    def forward(side, i):
        return pltpu.make_async_remote_copy(
            src_ref=hbuf.at[side, 0, pl.ds(i * PIECE, PIECE), :],
            dst_ref=hbuf.at[side, 1, pl.ds(i * PIECE, PIECE), :],
            send_sem=fwd_send.at[side, i],
            recv_sem=fwd_recv.at[side, i],
            device_id=(lat, other),
            device_id_type=MESH,
        )

    for i in range(pieces):

        @pl.when(has_high)
        def _():
            crossing(0, i).start()

        @pl.when(has_low)
        def _():
            crossing(1, i).start()

    pairs = tiles // 2
    given = [
        (wq_ref, wq2),
        (wk_ref, wk2),
        (bias_ref.at[pl.ds(other * pairs, pairs)], bias2),
        (wv_ref, wv2),
        (wo_ref, wo2),
        (gain_ref, gain2),
    ]
    gifts = [
        pltpu.make_async_remote_copy(
            src_ref=source,
            dst_ref=target,
            send_sem=w_send.at[i],
            recv_sem=w_recv.at[i],
            device_id=(lat, other),
            device_id_type=MESH,
        )
        for i, (source, target) in enumerate(given)
    ]
    for gift in gifts:
        gift.start()

    mesh_rows = mesh_ref[pl.ds(pl.multiple_of(c * half, half), half), :]

    def absorbed(part, wq, wk):
        q = jnp.dot(mesh_rows, wq[...], preferred_element_type=F32).astype(BF16)
        for j in range(2):
            s = slice(j * HEAD_DIM, (j + 1) * HEAD_DIM)
            qk = lax.dot_general(q[:, s], wk[:, s], NT, preferred_element_type=F32)
            qs[2 * part + j] = (qk * HEAD_DIM ** -0.5).astype(BF16)

    flat = table.reshape(table.shape[0] * 4, 128)

    def convert(rows, at, count):
        for col in range(4):
            flat[pl.ds(at * 4 + col, count, stride=4), :] = rows[:, col * 128:(col + 1) * 128].astype(F32)

    absorbed(0, wq_ref, wk_ref)
    for i in range(chunks):
        loads[i].wait()
        convert(buf.at[pl.ds(i * CH, CH), :], HALO + i * CH, CH)
    for gift in gifts:
        gift.wait()
    absorbed(1, wq2, wk2)

    side_rows = (0, HALO + band)

    def arrive(side, i):
        crossing(side, i).wait_recv()
        forward(side, i).start()
        convert(hbuf.at[side, 0, pl.ds(i * PIECE, PIECE), :], side_rows[side] + i * PIECE, PIECE)

    def arrive_forwarded(side, i):
        forward(side, i).wait()
        convert(hbuf.at[side, 1, pl.ds(i * PIECE, PIECE), :], side_rows[side] + share + i * PIECE, PIECE)

    for i in range(pieces + 1):
        for side, has in ((0, has_low), (1, has_high)):
            if i < pieces:
                pl.when(has)(functools.partial(arrive, side, i))
        for side, has in ((0, has_low), (1, has_high)):
            if i > 0:
                pl.when(has)(functools.partial(arrive_forwarded, side, i - 1))

    first_edge = c * (tiles * EDGES)
    node = lax.broadcasted_iota(jnp.int32, (TN, EDGES), 0)
    lane = lax.broadcasted_iota(jnp.int32, (TN, EDGES), 1)
    same = (lane % TN) == node

    def gather(t, st):
        for p in range(EDGES):
            st[p] = table[idx_ref[first_edge + t * EDGES + p]]

    def scores(t, st):
        st = st.reshape(EDGES * 4, 128)
        g = jnp.concatenate([st[pl.ds(col, EDGES, stride=4), :].astype(BF16) for col in range(4)], axis=1)
        gs[pl.ds(pl.multiple_of(t * EDGES, EDGES), EDGES), :] = g
        r0 = pl.multiple_of(t * TN, TN)
        qt = jnp.concatenate([qs[h, pl.ds(r0, TN), :] for h in range(HEADS)], axis=0)
        sc = lax.dot_general(qt, g, NT, preferred_element_type=F32)
        return [jnp.sum(jnp.where(same, sc[h * TN:(h + 1) * TN], 0.0), axis=0, keepdims=True) for h in range(HEADS)]

    gather(0, st0)

    @pl.loop(0, pairs)
    def _(i):
        t = 2 * i
        gather(t + 1, st1)
        s0 = scores(t, st0)
        gather(jnp.minimum(t + 2, tiles - 1), st0)
        s1 = scores(t + 1, st1)
        ss[i] = jnp.concatenate(s0[0:2] + s1[0:2] + s0[2:4] + s1[2:4], axis=0)

    blocks = EDGES // 128

    def fold(x, op):
        y = x[..., 0:128]
        for j in range(1, blocks):
            y = op(y, x[..., j * 128:(j + 1) * 128])
        y = op(y, pltpu.roll(y, 64, y.ndim - 1))
        return op(y, pltpu.roll(y, 32, y.ndim - 1))

    mine = bias_ref[pl.ds(c * pairs, pairs)]
    bias = jnp.concatenate([mine, bias2[...]], axis=1)
    s = ss[...] + bias
    m = fold(s, jnp.maximum)
    w = jnp.exp(s - jnp.concatenate([m] * blocks, axis=2))
    total = fold(w, jnp.add)
    ss[...] = w * jnp.concatenate([1.0 / total] * blocks, axis=2)

    @pl.loop(0, pairs)
    def _(i):
        both = ss[i]
        for j in range(2):
            t = 2 * i + j
            rows = [both[part * 4 + j * 2 + h:part * 4 + j * 2 + h + 1] for part in range(2) for h in range(2)]
            pt = jnp.concatenate([jnp.where(same, row, 0.0).astype(BF16) for row in rows], axis=0)
            g = gs[pl.ds(pl.multiple_of(t * EDGES, EDGES), EDGES), :]
            ctx = jnp.dot(pt, g, preferred_element_type=F32)
            r0 = pl.multiple_of(t * TN, TN)
            for h in range(HEADS):
                cs[h, pl.ds(r0, TN), :] = ctx[h * TN:(h + 1) * TN].astype(BF16)

    projected = jnp.zeros((half, D), F32)
    for part, (wv, wo) in enumerate(((wv_ref, wo_ref), (wv2, wo2))):
        attended = [
            jnp.dot(cs[2 * part + j], wv[:, j * HEAD_DIM:(j + 1) * HEAD_DIM], preferred_element_type=F32).astype(BF16)
            for j in range(2)
        ]
        projected = projected + jnp.dot(jnp.concatenate(attended, axis=1), wo[...], preferred_element_type=F32)
    updated = mesh_ref[pl.ds(pl.multiple_of(c * half, half), half), :].astype(F32) + projected
    mean = jnp.sum(updated, axis=1, keepdims=True) / D
    variance = jnp.sum(updated * updated, axis=1, keepdims=True) / D - mean * mean
    normed = (updated - mean) * lax.rsqrt(variance + EPSILON)
    left, right = normed[:, 0:D // 2], normed[:, D // 2:D]
    first = c == 0
    out_send[...] = (jnp.where(first, right, left) * gain2[0:1, :]).astype(BF16)
    swap = pltpu.make_async_remote_copy(
        src_ref=out_send,
        dst_ref=out_recv,
        send_sem=x_send,
        recv_sem=x_recv,
        device_id=(lat, other),
        device_id_type=MESH,
    )
    out_ref[pl.ds(pl.multiple_of(c * half, half), half), :] = (
        jnp.where(first, left, right) * gain_ref[0:1, :]
    ).astype(BF16)
    swap.start()
    swap.wait()
    out_ref[pl.ds(pl.multiple_of(other * half, half), half), :] = out_recv[...]
    for side, has in ((0, has_high), (1, has_low)):
        for i in range(pieces):

            @pl.when(has)
            def _():
                crossing(side, i).wait_send()


def shards(
    grid_latent, mesh_latent, neighbours, edge_bias, query_weight, key_weight, value_weight, out_weight, norm_gain
):
    band = grid_latent.shape[0]
    count = mesh_latent.shape[0]
    half = count // 2
    tiles = half // TN
    pieces = HALO // 2 // PIECE
    width = D // 2
    c = lax.axis_index("head")
    local = neighbours - (lax.axis_index("lat") * band - HALO)
    halo = (local < HALO) | (local >= HALO + band)
    row = jnp.where(halo, local ^ (c * (HALO // 2)), local)
    row = jnp.where(neighbours >= 0, row, HALO)
    idx = row.reshape(2 * tiles, TN, K).transpose(0, 2, 1).reshape(-1)
    live = (neighbours >= 0)[:, None, :]
    bias = jnp.where(live, edge_bias.astype(F32).reshape(count, 2, K), DEAD)
    bias = bias.reshape(tiles, 2, TN, 2, K).transpose(0, 1, 3, 4, 2).reshape(tiles, 4, EDGES)
    gain = jnp.broadcast_to(norm_gain.astype(F32)[None], (8, width))
    dma = pltpu.SemaphoreType.DMA
    out = pl.pallas_call(
        functools.partial(kernel, lax.axis_size("lat") - 1),
        out_shape=jax.ShapeDtypeStruct((count, width), BF16),
        in_specs=[ANY, SMEM] + [VMEM] * 7,
        out_specs=VMEM,
        scratch_shapes=[
            pltpu.VMEM((band, D), BF16),
            pltpu.VMEM((2, 2, HALO // 2, D), BF16),
            pltpu.VMEM((band + 2 * HALO, 4, 128), F32),
            pltpu.VMEM((EDGES, 4, 128), F32),
            pltpu.VMEM((EDGES, 4, 128), F32),
            pltpu.VMEM((HEADS, half, D), BF16),
            pltpu.VMEM((HEADS, half, D), BF16),
            pltpu.VMEM((tiles * EDGES, D), BF16),
            pltpu.VMEM((tiles // 2, 8, EDGES), F32),
            pltpu.VMEM((D, width), BF16),
            pltpu.VMEM((D, width), BF16),
            pltpu.VMEM((D, width), BF16),
            pltpu.VMEM((width, D), BF16),
            pltpu.VMEM((8, width), F32),
            pltpu.VMEM((tiles // 2, 4, EDGES), F32),
            pltpu.VMEM((half, width), BF16),
            pltpu.VMEM((half, width), BF16),
            dma((band // CH,)),
            dma((2, pieces)),
            dma((2, pieces)),
            dma((2, pieces)),
            dma((2, pieces)),
            dma((6,)),
            dma((6,)),
            dma,
            dma,
        ],
        compiler_params=pltpu.CompilerParams(
            collective_id=0, has_side_effects=True, vmem_limit_bytes=60 * 1024 * 1024
        ),
    )(grid_latent, idx, bias, mesh_latent, query_weight, key_weight, value_weight, out_weight, gain)
    return out


def solution(mesh):
    in_specs = (
        P("lat", None),
        P("lat", None),
        P("lat", None),
        P("lat", "head"),
        P(None, "head"),
        P(None, "head"),
        P(None, "head"),
        P("head", None),
        P("head"),
    )
    out_specs = P("lat", "head")
    return jax.shard_map(shards, mesh=mesh, in_specs=in_specs, out_specs=out_specs, check_vma=False)
```

```python
import functools

import jax
import jax.numpy as jnp
from jax import lax
from jax.experimental import pallas as pl
from jax.experimental.pallas import tpu as pltpu
from jax.sharding import PartitionSpec as P

D = 512
K = 16
HEADS = 4
HEAD_DIM = 128
HALO = 2048
EPSILON = 1e-05
TN = 32
EDGES = K * TN
CH = 512
PIECE = 256
DEAD = -1e30
VMEM = pl.BlockSpec(memory_space=pltpu.VMEM)
SMEM = pl.BlockSpec(memory_space=pltpu.SMEM)
ANY = pl.BlockSpec(memory_space=pl.ANY)
MESH = pl.DeviceIdType.MESH
NT = (((1,), (1,)), ((), ()))
F32 = jnp.float32
BF16 = jnp.bfloat16


def kernel(
    last, grid_ref, nb_ref, bias_ref, mesh_ref, wq_ref, wk_ref, wv_ref, wo_ref, gain_ref, out_ref,
    buf, hbuf, table, st0, st1, qs, cs, gs, ss, wq2, wk2, wv2, wo2, gain2, bias2, out_send, out_recv,
    channels, spread, rows_v, load_sem, ici_send, ici_recv, fwd_send, fwd_recv, w_send, w_recv, x_send, x_recv, s_sem,
    *row_refs,
):
    band = grid_ref.shape[0]
    half = mesh_ref.shape[0] // 2
    tiles = half // TN
    share = HALO // 2
    pieces = share // PIECE
    lat = lax.axis_index("lat")
    c = lax.axis_index("head")
    other = 1 - c
    has_low, has_high = lat > 0, lat < last
    below, above = jnp.maximum(lat - 1, 0), jnp.minimum(lat + 1, last)

    chunks = band // CH
    loads = [
        pltpu.make_async_copy(grid_ref.at[pl.ds(i * CH, CH), :], buf.at[pl.ds(i * CH, CH), :], load_sem.at[i])
        for i in range(chunks)
    ]
    for load in loads:
        load.start()

    barrier = pltpu.get_barrier_semaphore()
    pl.semaphore_signal(barrier, inc=1, device_id=(lat, other), device_id_type=MESH)

    @pl.when(has_low)
    def _():
        pl.semaphore_signal(barrier, inc=1, device_id=(below, c), device_id_type=MESH)

    @pl.when(has_high)
    def _():
        pl.semaphore_signal(barrier, inc=1, device_id=(above, c), device_id_type=MESH)

    pl.semaphore_wait(barrier, 1 + has_low.astype(jnp.int32) + has_high.astype(jnp.int32))

    def crossing(side, i):
        start = band - HALO if side == 0 else 0
        rows = pl.ds(pl.multiple_of(start + c * share + i * PIECE, PIECE), PIECE)
        return pltpu.make_async_remote_copy(
            src_ref=grid_ref.at[rows, :],
            dst_ref=hbuf.at[side, 0, pl.ds(i * PIECE, PIECE), :],
            send_sem=ici_send.at[side, i],
            recv_sem=ici_recv.at[side, i],
            device_id=(above if side == 0 else below, c),
            device_id_type=MESH,
        )

    def forward(side, i):
        return pltpu.make_async_remote_copy(
            src_ref=hbuf.at[side, 0, pl.ds(i * PIECE, PIECE), :],
            dst_ref=hbuf.at[side, 1, pl.ds(i * PIECE, PIECE), :],
            send_sem=fwd_send.at[side, i],
            recv_sem=fwd_recv.at[side, i],
            device_id=(lat, other),
            device_id_type=MESH,
        )

    for i in range(pieces):

        @pl.when(has_high)
        def _():
            crossing(0, i).start()

        @pl.when(has_low)
        def _():
            crossing(1, i).start()

    pairs = tiles // 2
    given = [
        (wq_ref, wq2),
        (wk_ref, wk2),
        (bias_ref, bias2),
        (wv_ref, wv2),
        (wo_ref, wo2),
        (gain_ref, gain2),
    ]
    gifts = [
        pltpu.make_async_remote_copy(
            src_ref=source,
            dst_ref=target,
            send_sem=w_send.at[i],
            recv_sem=w_recv.at[i],
            device_id=(lat, other),
            device_id_type=MESH,
        )
        for i, (source, target) in enumerate(given)
    ]
    for gift in gifts:
        gift.start()

    mesh_rows = mesh_ref[pl.ds(pl.multiple_of(c * half, half), half), :]

    def absorbed(part, wq, wk):
        q = jnp.dot(mesh_rows, wq[...], preferred_element_type=F32).astype(BF16)
        for j in range(2):
            s = slice(j * HEAD_DIM, (j + 1) * HEAD_DIM)
            qk = lax.dot_general(q[:, s], wk[:, s], NT, preferred_element_type=F32)
            qs[2 * part + j] = (qk * HEAD_DIM ** -0.5).astype(BF16)

    flat = table.reshape(table.shape[0] * 4, 128)

    def convert(rows, at, count):
        for col in range(4):
            flat[pl.ds(at * 4 + col, count, stride=4), :] = rows[:, col * 128:(col + 1) * 128].astype(F32)

    absorbed(0, wq_ref, wk_ref)
    for i in range(chunks):
        loads[i].wait()
        convert(buf.at[pl.ds(i * CH, CH), :], HALO + i * CH, CH)
    for gift in gifts:
        gift.wait()
    absorbed(1, wq2, wk2)

    node = lax.broadcasted_iota(jnp.int32, (TN, EDGES), 0)
    lane = lax.broadcasted_iota(jnp.int32, (TN, EDGES), 1)
    same = (lane % TN) == node

    nb = nb_ref[...]
    local = nb - (lat * band - HALO)
    live = nb >= 0
    at_end = (local < HALO) | (local >= HALO + band)
    row = jnp.where(live, jnp.where(at_end, local ^ (c * share), local), HALO)
    row = jnp.clip(row, 0, band + 2 * HALO - 1)
    stack = []
    for values in (bias_ref[...].astype(F32), bias2[...].astype(F32)):
        stack += [jnp.where(live, values[j * K:(j + 1) * K, :], DEAD) for j in range(2)]
    stack += [(row >> 6).astype(F32), (row & 63).astype(F32)]
    channels[...] = jnp.concatenate(stack, axis=0).T
    slot = lax.broadcasted_iota(jnp.int32, (K, EDGES), 0)
    slot_lane = lax.broadcasted_iota(jnp.int32, (K, EDGES), 1)
    place = jnp.where(slot_lane // TN == slot, 1.0, 0.0).astype(BF16)

    @pl.loop(0, pairs)
    def _(i):
        lines = []
        for j in range(2):
            r0 = pl.multiple_of(c * half + (2 * i + j) * TN, TN)
            mixed = channels[pl.ds(r0, TN), :]
            parts = jnp.concatenate([mixed[:, n * K:(n + 1) * K] for n in range(6)], axis=0).astype(BF16)
            wide = jnp.dot(parts, place, preferred_element_type=F32)
            line = [
                jnp.sum(jnp.where(same, wide[n * TN:(n + 1) * TN], 0.0), axis=0, keepdims=True) for n in range(6)
            ]
            rows_v[2 * i + j] = jnp.clip((line[4] * 64.0 + line[5]).astype(jnp.int32), 0, band + 2 * HALO - 1) * 4
            lines.append(line)
        spread[i] = jnp.concatenate(lines[0][0:2] + lines[1][0:2] + lines[0][2:4] + lines[1][2:4], axis=0)

    fetches = [pltpu.make_async_copy(rows_v.at[t], row_refs[t], s_sem.at[t]) for t in range(tiles)]
    for fetch in fetches:
        fetch.start()

    side_rows = (0, HALO + band)

    def arrive(side, i):
        crossing(side, i).wait_recv()
        forward(side, i).start()
        convert(hbuf.at[side, 0, pl.ds(i * PIECE, PIECE), :], side_rows[side] + i * PIECE, PIECE)

    def arrive_forwarded(side, i):
        forward(side, i).wait()
        convert(hbuf.at[side, 1, pl.ds(i * PIECE, PIECE), :], side_rows[side] + share + i * PIECE, PIECE)

    for i in range(pieces + 1):
        for side, has in ((0, has_low), (1, has_high)):
            if i < pieces:
                pl.when(has)(functools.partial(arrive, side, i))
        for side, has in ((0, has_low), (1, has_high)):
            if i > 0:
                pl.when(has)(functools.partial(arrive_forwarded, side, i - 1))

    for fetch in fetches:
        fetch.wait()

    def gather(t, st):
        for p in range(EDGES):
            st[p] = flat[pl.ds(row_refs[t][0, p], 4), :]

    def scores(t, st):
        st = st.reshape(EDGES * 4, 128)
        g = jnp.concatenate([st[pl.ds(col, EDGES, stride=4), :].astype(BF16) for col in range(4)], axis=1)
        gs[t * EDGES:(t + 1) * EDGES, :] = g
        qt = jnp.concatenate([qs[h, t * TN:(t + 1) * TN, :] for h in range(HEADS)], axis=0)
        sc = lax.dot_general(qt, g, NT, preferred_element_type=F32)
        return [jnp.sum(jnp.where(same, sc[h * TN:(h + 1) * TN], 0.0), axis=0, keepdims=True) for h in range(HEADS)]

    stages = (st0, st1)
    gather(0, st0)
    lines = []
    for t in range(tiles):
        if t + 1 < tiles:
            gather(t + 1, stages[(t + 1) % 2])
        lines.append(scores(t, stages[t % 2]))
        if t % 2:
            s0, s1 = lines[t - 1], lines[t]
            ss[t // 2] = jnp.concatenate(s0[0:2] + s1[0:2] + s0[2:4] + s1[2:4], axis=0)

    blocks = EDGES // 128

    def fold(x, op):
        y = x[..., 0:128]
        for j in range(1, blocks):
            y = op(y, x[..., j * 128:(j + 1) * 128])
        y = op(y, pltpu.roll(y, 64, y.ndim - 1))
        return op(y, pltpu.roll(y, 32, y.ndim - 1))

    s = ss[...] + spread[...]
    m = fold(s, jnp.maximum)
    w = jnp.exp(s - jnp.concatenate([m] * blocks, axis=2))
    total = fold(w, jnp.add)
    ss[...] = w * jnp.concatenate([1.0 / total] * blocks, axis=2)

    @pl.loop(0, pairs)
    def _(i):
        both = ss[i]
        for j in range(2):
            t = 2 * i + j
            rows = [both[part * 4 + j * 2 + h:part * 4 + j * 2 + h + 1] for part in range(2) for h in range(2)]
            pt = jnp.concatenate([jnp.where(same, row, 0.0).astype(BF16) for row in rows], axis=0)
            g = gs[pl.ds(pl.multiple_of(t * EDGES, EDGES), EDGES), :]
            ctx = jnp.dot(pt, g, preferred_element_type=F32)
            r0 = pl.multiple_of(t * TN, TN)
            for h in range(HEADS):
                cs[h, pl.ds(r0, TN), :] = ctx[h * TN:(h + 1) * TN].astype(BF16)

    projected = jnp.zeros((half, D), F32)
    for part, (wv, wo) in enumerate(((wv_ref, wo_ref), (wv2, wo2))):
        attended = [
            jnp.dot(cs[2 * part + j], wv[:, j * HEAD_DIM:(j + 1) * HEAD_DIM], preferred_element_type=F32).astype(BF16)
            for j in range(2)
        ]
        projected = projected + jnp.dot(jnp.concatenate(attended, axis=1), wo[...], preferred_element_type=F32)
    updated = mesh_ref[pl.ds(pl.multiple_of(c * half, half), half), :].astype(F32) + projected
    mean = jnp.sum(updated, axis=1, keepdims=True) / D
    variance = jnp.sum(updated * updated, axis=1, keepdims=True) / D - mean * mean
    normed = (updated - mean) * lax.rsqrt(variance + EPSILON)
    left, right = normed[:, 0:D // 2], normed[:, D // 2:D]
    first = c == 0
    out_send[...] = (jnp.where(first, right, left) * gain2[...].astype(F32)).astype(BF16)
    swap = pltpu.make_async_remote_copy(
        src_ref=out_send,
        dst_ref=out_recv,
        send_sem=x_send,
        recv_sem=x_recv,
        device_id=(lat, other),
        device_id_type=MESH,
    )
    out_ref[pl.ds(pl.multiple_of(c * half, half), half), :] = (
        jnp.where(first, left, right) * gain_ref[...].astype(F32)
    )
    swap.start()
    swap.wait()
    out_ref[pl.ds(pl.multiple_of(other * half, half), half), :] = out_recv[...].astype(F32)
    for side, has in ((0, has_high), (1, has_low)):
        for i in range(pieces):

            @pl.when(has)
            def _():
                crossing(side, i).wait_send()


def shards(
    grid_latent, mesh_latent, neighbours, edge_bias, query_weight, key_weight, value_weight, out_weight, norm_gain
):
    band = grid_latent.shape[0]
    count = mesh_latent.shape[0]
    half = count // 2
    tiles = half // TN
    pieces = HALO // 2 // PIECE
    width = D // 2
    dma = pltpu.SemaphoreType.DMA
    out = pl.pallas_call(
        functools.partial(kernel, lax.axis_size("lat") - 1),
        out_shape=jax.ShapeDtypeStruct((count, width), F32),
        in_specs=[ANY] + [VMEM] * 8,
        out_specs=VMEM,
        scratch_shapes=[
            pltpu.VMEM((band, D), BF16),
            pltpu.VMEM((2, 2, HALO // 2, D), BF16),
            pltpu.VMEM((band + 2 * HALO, 4, 128), F32),
            pltpu.VMEM((EDGES, 4, 128), F32),
            pltpu.VMEM((EDGES, 4, 128), F32),
            pltpu.VMEM((HEADS, half, D), BF16),
            pltpu.VMEM((HEADS, half, D), BF16),
            pltpu.VMEM((tiles * EDGES, D), BF16),
            pltpu.VMEM((tiles // 2, 8, EDGES), F32),
            pltpu.VMEM((D, width), BF16),
            pltpu.VMEM((D, width), BF16),
            pltpu.VMEM((D, width), BF16),
            pltpu.VMEM((width, D), BF16),
            pltpu.VMEM((1, width), BF16),
            pltpu.VMEM((2 * K, count), BF16),
            pltpu.VMEM((half, width), BF16),
            pltpu.VMEM((half, width), BF16),
            pltpu.VMEM((count, 6 * K), F32),
            pltpu.VMEM((tiles // 2, 8, EDGES), F32),
            pltpu.VMEM((tiles, 1, EDGES), jnp.int32),
            dma((band // CH,)),
            dma((2, pieces)),
            dma((2, pieces)),
            dma((2, pieces)),
            dma((2, pieces)),
            dma((6,)),
            dma((6,)),
            dma,
            dma,
            dma((tiles,)),
        ]
        + [pltpu.SMEM((1, EDGES), jnp.int32)] * tiles,
        compiler_params=pltpu.CompilerParams(
            collective_id=0, has_side_effects=True, vmem_limit_bytes=60 * 1024 * 1024
        ),
    )(
        grid_latent, neighbours.T, edge_bias.T, mesh_latent, query_weight, key_weight, value_weight, out_weight,
        norm_gain.reshape(1, width),
    )
    return out.astype(BF16)


def solution(mesh):
    in_specs = (
        P("lat", None),
        P("lat", None),
        P("lat", None),
        P("lat", "head"),
        P(None, "head"),
        P(None, "head"),
        P(None, "head"),
        P("head", None),
        P("head"),
    )
    out_specs = P("lat", "head")
    return jax.shard_map(shards, mesh=mesh, in_specs=in_specs, out_specs=out_specs, check_vma=False)
```

```python
import functools

import jax
import jax.numpy as jnp
from jax import lax
from jax.experimental import pallas as pl
from jax.experimental.pallas import tpu as pltpu
from jax.sharding import PartitionSpec as P

D = 512
K = 16
HEADS = 4
HEAD_DIM = 128
HALO = 2048
EPSILON = 1e-05
TN = 32
EDGES = K * TN
CH = 512
PIECE = 256
DEAD = -1e30
VMEM = pl.BlockSpec(memory_space=pltpu.VMEM)
SMEM = pl.BlockSpec(memory_space=pltpu.SMEM)
ANY = pl.BlockSpec(memory_space=pl.ANY)
MESH = pl.DeviceIdType.MESH
NT = (((1,), (1,)), ((), ()))
F32 = jnp.float32
BF16 = jnp.bfloat16


def kernel(
    last, grid_ref, nb_in, bias_in, mesh_in, wq_in, wk_in, wv_in, wo_in, gain_in, out_ref,
    buf, hbuf, table, st0, st1, qs, cs, gs, ss, wq2, wk2, wv2, wo2, gain2, bias2, out_send, out_keep,
    nb_ref, bias_ref, mesh_ref, wq_ref, wk_ref, wv_ref, wo_ref, gain_ref, local_sem,
    channels, spread, rows_v, load_sem, ici_send, ici_recv, fwd_send, fwd_recv, w_send, w_recv, x_send, x_recv, s_sem,
    *row_refs,
):
    band = grid_ref.shape[0]
    half = mesh_in.shape[0] // 2
    tiles = half // TN
    share = HALO // 2
    pieces = share // PIECE
    lat = lax.axis_index("lat")
    c = lax.axis_index("head")
    other = 1 - c
    has_low, has_high = lat > 0, lat < last
    below, above = jnp.maximum(lat - 1, 0), jnp.minimum(lat + 1, last)

    chunks = band // CH
    loads = [
        pltpu.make_async_copy(grid_ref.at[pl.ds(i * CH, CH), :], buf.at[pl.ds(i * CH, CH), :], load_sem.at[i])
        for i in range(chunks)
    ]
    barrier = pltpu.get_barrier_semaphore()
    pl.semaphore_signal(barrier, inc=1, device_id=(lat, other), device_id_type=MESH)

    @pl.when(has_low)
    def _():
        pl.semaphore_signal(barrier, inc=1, device_id=(below, c), device_id_type=MESH)

    @pl.when(has_high)
    def _():
        pl.semaphore_signal(barrier, inc=1, device_id=(above, c), device_id_type=MESH)

    pl.semaphore_wait(barrier, 1 + has_low.astype(jnp.int32) + has_high.astype(jnp.int32))

    def crossing(side, i):
        start = band - HALO if side == 0 else 0
        rows = pl.ds(pl.multiple_of(start + c * share + i * PIECE, PIECE), PIECE)
        return pltpu.make_async_remote_copy(
            src_ref=grid_ref.at[rows, :],
            dst_ref=hbuf.at[side, 0, pl.ds(i * PIECE, PIECE), :],
            send_sem=ici_send.at[side, i],
            recv_sem=ici_recv.at[side, i],
            device_id=(above if side == 0 else below, c),
            device_id_type=MESH,
        )

    def forward(side, i):
        return pltpu.make_async_remote_copy(
            src_ref=hbuf.at[side, 0, pl.ds(i * PIECE, PIECE), :],
            dst_ref=hbuf.at[side, 1, pl.ds(i * PIECE, PIECE), :],
            send_sem=fwd_send.at[side, i],
            recv_sem=fwd_recv.at[side, i],
            device_id=(lat, other),
            device_id_type=MESH,
        )

    for i in range(pieces):

        @pl.when(has_high)
        def _():
            crossing(0, i).start()

        @pl.when(has_low)
        def _():
            crossing(1, i).start()

    pairs = tiles // 2
    given = [
        (wq_in, wq2),
        (wk_in, wk2),
        (bias_in, bias2),
        (wv_in, wv2),
        (wo_in, wo2),
        (gain_in, gain2),
    ]
    gifts = [
        pltpu.make_async_remote_copy(
            src_ref=source,
            dst_ref=target,
            send_sem=w_send.at[i],
            recv_sem=w_recv.at[i],
            device_id=(lat, other),
            device_id_type=MESH,
        )
        for i, (source, target) in enumerate(given)
    ]
    for gift in gifts:
        gift.start()
    mine = [
        (mesh_in.at[pl.ds(pl.multiple_of(c * half, half), half), :], mesh_ref),
        (wq_in, wq_ref),
        (wk_in, wk_ref),
        (nb_in, nb_ref),
        (bias_in, bias_ref),
        (wv_in, wv_ref),
        (wo_in, wo_ref),
        (gain_in, gain_ref),
    ]
    mine = [pltpu.make_async_copy(source, target, local_sem.at[i]) for i, (source, target) in enumerate(mine)]
    for load in mine + loads:
        load.start()
    for load in mine:
        load.wait()

    mesh_rows = mesh_ref[...]

    def absorbed(part, wq, wk):
        q = jnp.dot(mesh_rows, wq[...], preferred_element_type=F32).astype(BF16)
        for j in range(2):
            s = slice(j * HEAD_DIM, (j + 1) * HEAD_DIM)
            qk = lax.dot_general(q[:, s], wk[:, s], NT, preferred_element_type=F32)
            qs[2 * part + j] = (qk * HEAD_DIM ** -0.5).astype(BF16)

    flat = table.reshape(table.shape[0] * 4, 128)

    def convert(rows, at, count):
        for col in range(4):
            flat[pl.ds(at * 4 + col, count, stride=4), :] = rows[:, col * 128:(col + 1) * 128].astype(F32)

    absorbed(0, wq_ref, wk_ref)
    for i in range(chunks):
        loads[i].wait()
        convert(buf.at[pl.ds(i * CH, CH), :], HALO + i * CH, CH)
    for gift in gifts:
        gift.wait()
    absorbed(1, wq2, wk2)

    node = lax.broadcasted_iota(jnp.int32, (TN, EDGES), 0)
    lane = lax.broadcasted_iota(jnp.int32, (TN, EDGES), 1)
    same = (lane % TN) == node

    nb = nb_ref[...]
    local = nb - (lat * band - HALO)
    live = nb >= 0
    at_end = (local < HALO) | (local >= HALO + band)
    row = jnp.where(live, jnp.where(at_end, local ^ (c * share), local), HALO)
    row = jnp.clip(row, 0, band + 2 * HALO - 1)
    stack = []
    for values in (bias_ref[...].astype(F32), bias2[...].astype(F32)):
        stack += [jnp.where(live, values[j * K:(j + 1) * K, :], DEAD) for j in range(2)]
    stack += [(row >> 6).astype(F32), (row & 63).astype(F32)]
    channels[...] = jnp.concatenate(stack, axis=0).T
    slot = lax.broadcasted_iota(jnp.int32, (K, EDGES), 0)
    slot_lane = lax.broadcasted_iota(jnp.int32, (K, EDGES), 1)
    place = jnp.where(slot_lane // TN == slot, 1.0, 0.0).astype(BF16)

    @pl.loop(0, pairs)
    def _(i):
        lines = []
        for j in range(2):
            r0 = pl.multiple_of(c * half + (2 * i + j) * TN, TN)
            mixed = channels[pl.ds(r0, TN), :]
            parts = jnp.concatenate([mixed[:, n * K:(n + 1) * K] for n in range(6)], axis=0).astype(BF16)
            wide = jnp.dot(parts, place, preferred_element_type=F32)
            line = [
                jnp.sum(jnp.where(same, wide[n * TN:(n + 1) * TN], 0.0), axis=0, keepdims=True) for n in range(6)
            ]
            rows_v[2 * i + j] = jnp.clip((line[4] * 64.0 + line[5]).astype(jnp.int32), 0, band + 2 * HALO - 1) * 4
            lines.append(line)
        spread[i] = jnp.concatenate(lines[0][0:2] + lines[1][0:2] + lines[0][2:4] + lines[1][2:4], axis=0)

    fetches = [pltpu.make_async_copy(rows_v.at[t], row_refs[t], s_sem.at[t]) for t in range(tiles)]
    for fetch in fetches:
        fetch.start()

    side_rows = (0, HALO + band)

    def arrive(side, i):
        crossing(side, i).wait_recv()
        forward(side, i).start()
        convert(hbuf.at[side, 0, pl.ds(i * PIECE, PIECE), :], side_rows[side] + i * PIECE, PIECE)

    def arrive_forwarded(side, i):
        forward(side, i).wait()
        convert(hbuf.at[side, 1, pl.ds(i * PIECE, PIECE), :], side_rows[side] + share + i * PIECE, PIECE)

    for i in range(pieces + 1):
        for side, has in ((0, has_low), (1, has_high)):
            if i < pieces:
                pl.when(has)(functools.partial(arrive, side, i))
        for side, has in ((0, has_low), (1, has_high)):
            if i > 0:
                pl.when(has)(functools.partial(arrive_forwarded, side, i - 1))

    for fetch in fetches:
        fetch.wait()

    def gather(t, st):
        for p in range(EDGES):
            st[p] = flat[pl.ds(row_refs[t][0, p], 4), :]

    def scores(t, st):
        st = st.reshape(EDGES * 4, 128)
        g = jnp.concatenate([st[pl.ds(col, EDGES, stride=4), :].astype(BF16) for col in range(4)], axis=1)
        gs[t * EDGES:(t + 1) * EDGES, :] = g
        qt = jnp.concatenate([qs[h, t * TN:(t + 1) * TN, :] for h in range(HEADS)], axis=0)
        sc = lax.dot_general(qt, g, NT, preferred_element_type=F32)
        return [jnp.sum(jnp.where(same, sc[h * TN:(h + 1) * TN], 0.0), axis=0, keepdims=True) for h in range(HEADS)]

    stages = (st0, st1)
    gather(0, st0)
    lines = []
    for t in range(tiles):
        if t + 1 < tiles:
            gather(t + 1, stages[(t + 1) % 2])
        lines.append(scores(t, stages[t % 2]))
        if t % 2:
            s0, s1 = lines[t - 1], lines[t]
            ss[t // 2] = jnp.concatenate(s0[0:2] + s1[0:2] + s0[2:4] + s1[2:4], axis=0)

    blocks = EDGES // 128

    def fold(x, op):
        y = x[..., 0:128]
        for j in range(1, blocks):
            y = op(y, x[..., j * 128:(j + 1) * 128])
        y = op(y, pltpu.roll(y, 64, y.ndim - 1))
        return op(y, pltpu.roll(y, 32, y.ndim - 1))

    s = ss[...] + spread[...]
    m = fold(s, jnp.maximum)
    w = jnp.exp(s - jnp.concatenate([m] * blocks, axis=2))
    total = fold(w, jnp.add)
    ss[...] = w * jnp.concatenate([1.0 / total] * blocks, axis=2)

    @pl.loop(0, pairs)
    def _(i):
        both = ss[i]
        for j in range(2):
            t = 2 * i + j
            rows = [both[part * 4 + j * 2 + h:part * 4 + j * 2 + h + 1] for part in range(2) for h in range(2)]
            pt = jnp.concatenate([jnp.where(same, row, 0.0).astype(BF16) for row in rows], axis=0)
            g = gs[pl.ds(pl.multiple_of(t * EDGES, EDGES), EDGES), :]
            ctx = jnp.dot(pt, g, preferred_element_type=F32)
            r0 = pl.multiple_of(t * TN, TN)
            for h in range(HEADS):
                cs[h, pl.ds(r0, TN), :] = ctx[h * TN:(h + 1) * TN].astype(BF16)

    projected = jnp.zeros((half, D), F32)
    for part, (wv, wo) in enumerate(((wv_ref, wo_ref), (wv2, wo2))):
        attended = [
            jnp.dot(cs[2 * part + j], wv[:, j * HEAD_DIM:(j + 1) * HEAD_DIM], preferred_element_type=F32).astype(BF16)
            for j in range(2)
        ]
        projected = projected + jnp.dot(jnp.concatenate(attended, axis=1), wo[...], preferred_element_type=F32)
    updated = mesh_ref[...].astype(F32) + projected
    mean = jnp.sum(updated, axis=1, keepdims=True) / D
    variance = jnp.sum(updated * updated, axis=1, keepdims=True) / D - mean * mean
    normed = (updated - mean) * lax.rsqrt(variance + EPSILON)
    left, right = normed[:, 0:D // 2], normed[:, D // 2:D]
    first = c == 0
    gains = [gain_ref[...].astype(F32).reshape(1, D // 2), gain2[...].astype(F32).reshape(1, D // 2)]
    out_send[...] = (jnp.where(first, right, left) * gains[1]).astype(BF16)
    out_keep[...] = (jnp.where(first, left, right) * gains[0]).astype(BF16)
    out_rows = out_ref.at[pl.ds(pl.multiple_of(c * half, half), half), :]
    swap = pltpu.make_async_remote_copy(
        src_ref=out_send,
        dst_ref=out_rows,
        send_sem=x_send,
        recv_sem=x_recv,
        device_id=(lat, other),
        device_id_type=MESH,
    )
    swap.start()
    keep = pltpu.make_async_copy(out_keep, out_rows, local_sem.at[0])
    keep.start()
    keep.wait()
    swap.wait()
    for side, has in ((0, has_high), (1, has_low)):
        for i in range(pieces):

            @pl.when(has)
            def _():
                crossing(side, i).wait_send()


def shards(
    grid_latent, mesh_latent, neighbours, edge_bias, query_weight, key_weight, value_weight, out_weight, norm_gain
):
    band = grid_latent.shape[0]
    count = mesh_latent.shape[0]
    half = count // 2
    tiles = half // TN
    pieces = HALO // 2 // PIECE
    width = D // 2
    dma = pltpu.SemaphoreType.DMA
    out = pl.pallas_call(
        functools.partial(kernel, lax.axis_size("lat") - 1),
        out_shape=jax.ShapeDtypeStruct((count, width), BF16),
        in_specs=[ANY] * 9,
        out_specs=ANY,
        scratch_shapes=[
            pltpu.VMEM((band, D), BF16),
            pltpu.VMEM((2, 2, HALO // 2, D), BF16),
            pltpu.VMEM((band + 2 * HALO, 4, 128), F32),
            pltpu.VMEM((EDGES, 4, 128), F32),
            pltpu.VMEM((EDGES, 4, 128), F32),
            pltpu.VMEM((HEADS, half, D), BF16),
            pltpu.VMEM((HEADS, half, D), BF16),
            pltpu.VMEM((tiles * EDGES, D), BF16),
            pltpu.VMEM((tiles // 2, 8, EDGES), F32),
            pltpu.VMEM((D, width), BF16),
            pltpu.VMEM((D, width), BF16),
            pltpu.VMEM((D, width), BF16),
            pltpu.VMEM((width, D), BF16),
            pltpu.VMEM((width,), BF16),
            pltpu.VMEM((2 * K, count), BF16),
            pltpu.VMEM((half, width), BF16),
            pltpu.VMEM((half, width), BF16),
            pltpu.VMEM((K, count), jnp.int32),
            pltpu.VMEM((2 * K, count), BF16),
            pltpu.VMEM((half, D), BF16),
            pltpu.VMEM((D, width), BF16),
            pltpu.VMEM((D, width), BF16),
            pltpu.VMEM((D, width), BF16),
            pltpu.VMEM((width, D), BF16),
            pltpu.VMEM((width,), BF16),
            dma((8,)),
            pltpu.VMEM((count, 6 * K), F32),
            pltpu.VMEM((tiles // 2, 8, EDGES), F32),
            pltpu.VMEM((tiles, 1, EDGES), jnp.int32),
            dma((band // CH,)),
            dma((2, pieces)),
            dma((2, pieces)),
            dma((2, pieces)),
            dma((2, pieces)),
            dma((6,)),
            dma((6,)),
            dma,
            dma,
            dma((tiles,)),
        ]
        + [pltpu.SMEM((1, EDGES), jnp.int32)] * tiles,
        compiler_params=pltpu.CompilerParams(
            collective_id=0, has_side_effects=True, vmem_limit_bytes=60 * 1024 * 1024
        ),
    )(
        grid_latent, neighbours.T, edge_bias.T, mesh_latent, query_weight, key_weight, value_weight, out_weight,
        norm_gain,
    )
    return out


def solution(mesh):
    in_specs = (
        P("lat", None),
        P("lat", None),
        P("lat", None),
        P("lat", "head"),
        P(None, "head"),
        P(None, "head"),
        P(None, "head"),
        P("head", None),
        P("head"),
    )
    out_specs = P("lat", "head")
    return jax.shard_map(shards, mesh=mesh, in_specs=in_specs, out_specs=out_specs, check_vma=False)
```

```python
import functools

import jax
import jax.numpy as jnp
from jax import lax
from jax.experimental import pallas as pl
from jax.experimental.pallas import tpu as pltpu
from jax.sharding import PartitionSpec as P

D = 512
K = 16
HEADS = 4
HEAD_DIM = 128
HALO = 2048
EPSILON = 1e-05
TN = 32
EDGES = K * TN
CH = 512
PIECE = 256
DEAD = -1e30
VMEM = pl.BlockSpec(memory_space=pltpu.VMEM)
SMEM = pl.BlockSpec(memory_space=pltpu.SMEM)
ANY = pl.BlockSpec(memory_space=pl.ANY)
MESH = pl.DeviceIdType.MESH
NT = (((1,), (1,)), ((), ()))
F32 = jnp.float32
BF16 = jnp.bfloat16


def kernel(
    last, grid_ref, nb_in, bias_in, mesh_in, wq_in, wk_in, wv_in, wo_in, gain_in, out_ref,
    buf, hbuf, table, st0, st1, qs, cs, gs, ss, wq2, wk2, wv2, wo2, gain2, bias2, out_send, out_keep,
    nb_ref, bias_ref, mesh_ref, wq_ref, wk_ref, wv_ref, wo_ref, gain_ref, local_sem,
    channels, spread, rows_v, load_sem, ici_send, ici_recv, fwd_send, fwd_recv, w_send, w_recv, x_send, x_recv, s_sem,
    *row_refs,
):
    band = grid_ref.shape[0]
    half = mesh_in.shape[0] // 2
    tiles = half // TN
    share = HALO // 2
    pieces = share // PIECE
    lat = lax.axis_index("lat")
    c = lax.axis_index("head")
    other = 1 - c
    has_low, has_high = lat > 0, lat < last
    below, above = jnp.maximum(lat - 1, 0), jnp.minimum(lat + 1, last)

    chunks = band // CH
    loads = [
        pltpu.make_async_copy(grid_ref.at[pl.ds(i * CH, CH), :], buf.at[pl.ds(i * CH, CH), :], load_sem.at[i])
        for i in range(chunks)
    ]
    barrier = pltpu.get_barrier_semaphore()
    pl.semaphore_signal(barrier, inc=1, device_id=(lat, other), device_id_type=MESH)

    @pl.when(has_low)
    def _():
        pl.semaphore_signal(barrier, inc=1, device_id=(below, c), device_id_type=MESH)

    @pl.when(has_high)
    def _():
        pl.semaphore_signal(barrier, inc=1, device_id=(above, c), device_id_type=MESH)

    pl.semaphore_wait(barrier, 1 + has_low.astype(jnp.int32) + has_high.astype(jnp.int32))

    def crossing(side, i):
        start = band - HALO if side == 0 else 0
        rows = pl.ds(pl.multiple_of(start + c * share + i * PIECE, PIECE), PIECE)
        return pltpu.make_async_remote_copy(
            src_ref=grid_ref.at[rows, :],
            dst_ref=hbuf.at[side, 0, pl.ds(i * PIECE, PIECE), :],
            send_sem=ici_send.at[side, i],
            recv_sem=ici_recv.at[side, i],
            device_id=(above if side == 0 else below, c),
            device_id_type=MESH,
        )

    def forward(side, i):
        return pltpu.make_async_remote_copy(
            src_ref=hbuf.at[side, 0, pl.ds(i * PIECE, PIECE), :],
            dst_ref=hbuf.at[side, 1, pl.ds(i * PIECE, PIECE), :],
            send_sem=fwd_send.at[side, i],
            recv_sem=fwd_recv.at[side, i],
            device_id=(lat, other),
            device_id_type=MESH,
        )

    for i in range(pieces):

        @pl.when(has_high)
        def _():
            crossing(0, i).start()

        @pl.when(has_low)
        def _():
            crossing(1, i).start()

    pairs = tiles // 2
    given = [
        (wq_in, wq2),
        (wk_in, wk2),
        (bias_in, bias2),
        (wv_in, wv2),
        (wo_in, wo2),
        (gain_in, gain2),
    ]
    gifts = [
        pltpu.make_async_remote_copy(
            src_ref=source,
            dst_ref=target,
            send_sem=w_send.at[i],
            recv_sem=w_recv.at[i],
            device_id=(lat, other),
            device_id_type=MESH,
        )
        for i, (source, target) in enumerate(given)
    ]
    for gift in gifts:
        gift.start()
    mine = [
        (mesh_in.at[pl.ds(pl.multiple_of(c * half, half), half), :], mesh_ref),
        (wq_in, wq_ref),
        (wk_in, wk_ref),
        (nb_in, nb_ref),
        (bias_in, bias_ref),
        (wv_in, wv_ref),
        (wo_in, wo_ref),
        (gain_in, gain_ref),
    ]
    mine = [pltpu.make_async_copy(source, target, local_sem.at[i]) for i, (source, target) in enumerate(mine)]
    for load in mine + loads:
        load.start()
    for load in mine:
        load.wait()

    mesh_rows = mesh_ref[...]

    def absorbed(part, wq, wk):
        q = jnp.dot(mesh_rows, wq[...], preferred_element_type=F32).astype(BF16)
        for j in range(2):
            s = slice(j * HEAD_DIM, (j + 1) * HEAD_DIM)
            qk = lax.dot_general(q[:, s], wk[:, s], NT, preferred_element_type=F32)
            qs[2 * part + j] = (qk * HEAD_DIM ** -0.5).astype(BF16)

    flat = table.reshape(table.shape[0] * 4, 128)

    def convert(rows, at, count):
        for col in range(4):
            flat[pl.ds(at * 4 + col, count, stride=4), :] = rows[:, col * 128:(col + 1) * 128].astype(F32)

    absorbed(0, wq_ref, wk_ref)
    for i in range(chunks):
        loads[i].wait()
        convert(buf.at[pl.ds(i * CH, CH), :], HALO + i * CH, CH)
    for gift in gifts:
        gift.wait()
    absorbed(1, wq2, wk2)

    node = lax.broadcasted_iota(jnp.int32, (TN, EDGES), 0)
    lane = lax.broadcasted_iota(jnp.int32, (TN, EDGES), 1)
    same = (lane % TN) == node

    nb = nb_ref[...]
    local = nb - (lat * band - HALO)
    live = nb >= 0
    at_end = (local < HALO) | (local >= HALO + band)
    row = jnp.where(live, jnp.where(at_end, local ^ (c * share), local), HALO)
    row = jnp.clip(row, 0, band + 2 * HALO - 1)
    stack = []
    for values in (bias_ref[...].astype(F32), bias2[...].astype(F32)):
        stack += [jnp.where(live, values[j * K:(j + 1) * K, :], DEAD) for j in range(2)]
    stack += [(row >> 6).astype(F32), (row & 63).astype(F32)]
    channels[...] = jnp.concatenate(stack, axis=0).T
    slot = lax.broadcasted_iota(jnp.int32, (K, EDGES), 0)
    slot_lane = lax.broadcasted_iota(jnp.int32, (K, EDGES), 1)
    place = jnp.where(slot_lane // TN == slot, 1.0, 0.0).astype(BF16)

    @pl.loop(0, pairs)
    def _(i):
        lines = []
        for j in range(2):
            r0 = pl.multiple_of(c * half + (2 * i + j) * TN, TN)
            mixed = channels[pl.ds(r0, TN), :]
            parts = jnp.concatenate([mixed[:, n * K:(n + 1) * K] for n in range(6)], axis=0).astype(BF16)
            wide = jnp.dot(parts, place, preferred_element_type=F32)
            line = [
                jnp.sum(jnp.where(same, wide[n * TN:(n + 1) * TN], 0.0), axis=0, keepdims=True) for n in range(6)
            ]
            rows_v[2 * i + j] = jnp.clip((line[4] * 64.0 + line[5]).astype(jnp.int32), 0, band + 2 * HALO - 1) * 4
            lines.append(line)
        spread[i] = jnp.concatenate(lines[0][0:2] + lines[1][0:2] + lines[0][2:4] + lines[1][2:4], axis=0)

    fetches = [pltpu.make_async_copy(rows_v.at[t], row_refs[t], s_sem.at[t]) for t in range(tiles)]
    for fetch in fetches:
        fetch.start()

    side_rows = (0, HALO + band)

    def arrive(side, i):
        crossing(side, i).wait_recv()
        forward(side, i).start()
        convert(hbuf.at[side, 0, pl.ds(i * PIECE, PIECE), :], side_rows[side] + i * PIECE, PIECE)

    def arrive_forwarded(side, i):
        forward(side, i).wait()
        convert(hbuf.at[side, 1, pl.ds(i * PIECE, PIECE), :], side_rows[side] + share + i * PIECE, PIECE)

    for i in range(pieces + 1):
        for side, has in ((0, has_low), (1, has_high)):
            if i < pieces:
                pl.when(has)(functools.partial(arrive, side, i))
        for side, has in ((0, has_low), (1, has_high)):
            if i > 0:
                pl.when(has)(functools.partial(arrive_forwarded, side, i - 1))

    for fetch in fetches:
        fetch.wait()

    def gather(t, st):
        for p in range(EDGES):
            st[p] = flat[pl.ds(row_refs[t][0, p], 4), :]

    def scores(t, st):
        st = st.reshape(EDGES * 4, 128)
        g = jnp.concatenate([st[pl.ds(col, EDGES, stride=4), :].astype(BF16) for col in range(4)], axis=1)
        gs[t * EDGES:(t + 1) * EDGES, :] = g
        qt = jnp.concatenate([qs[h, t * TN:(t + 1) * TN, :] for h in range(HEADS)], axis=0)
        sc = lax.dot_general(qt, g, NT, preferred_element_type=F32)
        return [jnp.sum(jnp.where(same, sc[h * TN:(h + 1) * TN], 0.0), axis=0, keepdims=True) for h in range(HEADS)]

    stages = (st0, st1)
    gather(0, st0)
    lines = []
    for t in range(tiles):
        if t + 1 < tiles:
            gather(t + 1, stages[(t + 1) % 2])
        lines.append(scores(t, stages[t % 2]))
        if t % 2:
            s0, s1 = lines[t - 1], lines[t]
            ss[t // 2] = jnp.concatenate(s0[0:2] + s1[0:2] + s0[2:4] + s1[2:4], axis=0)

    blocks = EDGES // 128

    def fold(x, op):
        y = x[..., 0:128]
        for j in range(1, blocks):
            y = op(y, x[..., j * 128:(j + 1) * 128])
        y = op(y, pltpu.roll(y, 64, y.ndim - 1))
        return op(y, pltpu.roll(y, 32, y.ndim - 1))

    s = ss[...] + spread[...]
    m = fold(s, jnp.maximum)
    w = jnp.exp(s - jnp.concatenate([m] * blocks, axis=2))
    total = fold(w, jnp.add)
    ss[...] = w * jnp.concatenate([1.0 / total] * blocks, axis=2)

    for i in range(pairs):
        both = ss[i]
        for j in range(2):
            t = 2 * i + j
            rows = [both[part * 4 + j * 2 + h:part * 4 + j * 2 + h + 1] for part in range(2) for h in range(2)]
            pt = jnp.concatenate([jnp.where(same, row, 0.0).astype(BF16) for row in rows], axis=0)
            g = gs[t * EDGES:(t + 1) * EDGES, :]
            ctx = jnp.dot(pt, g, preferred_element_type=F32)
            for h in range(HEADS):
                cs[h, t * TN:(t + 1) * TN, :] = ctx[h * TN:(h + 1) * TN].astype(BF16)

    projected = jnp.zeros((half, D), F32)
    for part, (wv, wo) in enumerate(((wv_ref, wo_ref), (wv2, wo2))):
        attended = [
            jnp.dot(cs[2 * part + j], wv[:, j * HEAD_DIM:(j + 1) * HEAD_DIM], preferred_element_type=F32).astype(BF16)
            for j in range(2)
        ]
        projected = projected + jnp.dot(jnp.concatenate(attended, axis=1), wo[...], preferred_element_type=F32)
    updated = mesh_ref[...].astype(F32) + projected
    mean = jnp.sum(updated, axis=1, keepdims=True) / D
    variance = jnp.sum(updated * updated, axis=1, keepdims=True) / D - mean * mean
    normed = (updated - mean) * lax.rsqrt(variance + EPSILON)
    left, right = normed[:, 0:D // 2], normed[:, D // 2:D]
    first = c == 0
    gains = [gain_ref[...].astype(F32).reshape(1, D // 2), gain2[...].astype(F32).reshape(1, D // 2)]
    out_send[...] = (jnp.where(first, right, left) * gains[1]).astype(BF16)
    out_keep[...] = (jnp.where(first, left, right) * gains[0]).astype(BF16)
    out_rows = out_ref.at[pl.ds(pl.multiple_of(c * half, half), half), :]
    swap = pltpu.make_async_remote_copy(
        src_ref=out_send,
        dst_ref=out_rows,
        send_sem=x_send,
        recv_sem=x_recv,
        device_id=(lat, other),
        device_id_type=MESH,
    )
    swap.start()
    keep = pltpu.make_async_copy(out_keep, out_rows, local_sem.at[0])
    keep.start()
    keep.wait()
    swap.wait()
    for side, has in ((0, has_high), (1, has_low)):
        for i in range(pieces):

            @pl.when(has)
            def _():
                crossing(side, i).wait_send()


def shards(
    grid_latent, mesh_latent, neighbours, edge_bias, query_weight, key_weight, value_weight, out_weight, norm_gain
):
    band = grid_latent.shape[0]
    count = mesh_latent.shape[0]
    half = count // 2
    tiles = half // TN
    pieces = HALO // 2 // PIECE
    width = D // 2
    dma = pltpu.SemaphoreType.DMA
    out = pl.pallas_call(
        functools.partial(kernel, lax.axis_size("lat") - 1),
        out_shape=jax.ShapeDtypeStruct((count, width), BF16),
        in_specs=[ANY] * 9,
        out_specs=ANY,
        scratch_shapes=[
            pltpu.VMEM((band, D), BF16),
            pltpu.VMEM((2, 2, HALO // 2, D), BF16),
            pltpu.VMEM((band + 2 * HALO, 4, 128), F32),
            pltpu.VMEM((EDGES, 4, 128), F32),
            pltpu.VMEM((EDGES, 4, 128), F32),
            pltpu.VMEM((HEADS, half, D), BF16),
            pltpu.VMEM((HEADS, half, D), BF16),
            pltpu.VMEM((tiles * EDGES, D), BF16),
            pltpu.VMEM((tiles // 2, 8, EDGES), F32),
            pltpu.VMEM((D, width), BF16),
            pltpu.VMEM((D, width), BF16),
            pltpu.VMEM((D, width), BF16),
            pltpu.VMEM((width, D), BF16),
            pltpu.VMEM((width,), BF16),
            pltpu.VMEM((2 * K, count), BF16),
            pltpu.VMEM((half, width), BF16),
            pltpu.VMEM((half, width), BF16),
            pltpu.VMEM((K, count), jnp.int32),
            pltpu.VMEM((2 * K, count), BF16),
            pltpu.VMEM((half, D), BF16),
            pltpu.VMEM((D, width), BF16),
            pltpu.VMEM((D, width), BF16),
            pltpu.VMEM((D, width), BF16),
            pltpu.VMEM((width, D), BF16),
            pltpu.VMEM((width,), BF16),
            dma((8,)),
            pltpu.VMEM((count, 6 * K), F32),
            pltpu.VMEM((tiles // 2, 8, EDGES), F32),
            pltpu.VMEM((tiles, 1, EDGES), jnp.int32),
            dma((band // CH,)),
            dma((2, pieces)),
            dma((2, pieces)),
            dma((2, pieces)),
            dma((2, pieces)),
            dma((6,)),
            dma((6,)),
            dma,
            dma,
            dma((tiles,)),
        ]
        + [pltpu.SMEM((1, EDGES), jnp.int32)] * tiles,
        compiler_params=pltpu.CompilerParams(
            collective_id=0, has_side_effects=True, vmem_limit_bytes=60 * 1024 * 1024
        ),
    )(
        grid_latent, neighbours.T, edge_bias.T, mesh_latent, query_weight, key_weight, value_weight, out_weight,
        norm_gain,
    )
    return out


def solution(mesh):
    in_specs = (
        P("lat", None),
        P("lat", None),
        P("lat", None),
        P("lat", "head"),
        P(None, "head"),
        P(None, "head"),
        P(None, "head"),
        P("head", None),
        P("head"),
    )
    out_specs = P("lat", "head")
    return jax.shard_map(shards, mesh=mesh, in_specs=in_specs, out_specs=out_specs, check_vma=False)
```

```python
import functools

import jax
import jax.numpy as jnp
from jax import lax
from jax.experimental import pallas as pl
from jax.experimental.pallas import tpu as pltpu
from jax.sharding import PartitionSpec as P

D = 512
K = 16
HEADS = 4
HEAD_DIM = 128
HALO = 2048
EPSILON = 1e-05
TN = 32
EDGES = K * TN
CH = 512
PIECE = 128
DEAD = -1e30
VMEM = pl.BlockSpec(memory_space=pltpu.VMEM)
SMEM = pl.BlockSpec(memory_space=pltpu.SMEM)
ANY = pl.BlockSpec(memory_space=pl.ANY)
MESH = pl.DeviceIdType.MESH
NT = (((1,), (1,)), ((), ()))
F32 = jnp.float32
BF16 = jnp.bfloat16


def kernel(
    last, grid_ref, nb_in, bias_in, mesh_in, wq_in, wk_in, wv_in, wo_in, gain_in, out_ref,
    buf, hbuf, table, st0, st1, qs, cs, gs, ss, wq2, wk2, wv2, wo2, gain2, bias2, out_send, out_keep,
    nb_ref, bias_ref, mesh_ref, wq_ref, wk_ref, wv_ref, wo_ref, gain_ref, local_sem,
    channels, spread, rows_v, load_sem, ici_send, ici_recv, fwd_send, fwd_recv, w_send, w_recv, x_send, x_recv, s_sem,
    *row_refs,
):
    band = grid_ref.shape[0]
    half = mesh_in.shape[0] // 2
    tiles = half // TN
    share = HALO // 2
    pieces = share // PIECE
    lat = lax.axis_index("lat")
    c = lax.axis_index("head")
    other = 1 - c
    has_low, has_high = lat > 0, lat < last
    below, above = jnp.maximum(lat - 1, 0), jnp.minimum(lat + 1, last)

    chunks = band // CH
    loads = [
        pltpu.make_async_copy(grid_ref.at[pl.ds(i * CH, CH), :], buf.at[pl.ds(i * CH, CH), :], load_sem.at[i])
        for i in range(chunks)
    ]
    barrier = pltpu.get_barrier_semaphore()
    pl.semaphore_signal(barrier, inc=1, device_id=(lat, other), device_id_type=MESH)

    @pl.when(has_low)
    def _():
        pl.semaphore_signal(barrier, inc=1, device_id=(below, c), device_id_type=MESH)

    @pl.when(has_high)
    def _():
        pl.semaphore_signal(barrier, inc=1, device_id=(above, c), device_id_type=MESH)

    pl.semaphore_wait(barrier, 1 + has_low.astype(jnp.int32) + has_high.astype(jnp.int32))

    def crossing(side, i):
        start = band - HALO if side == 0 else 0
        rows = pl.ds(pl.multiple_of(start + c * share + i * PIECE, PIECE), PIECE)
        return pltpu.make_async_remote_copy(
            src_ref=grid_ref.at[rows, :],
            dst_ref=hbuf.at[side, 0, pl.ds(i * PIECE, PIECE), :],
            send_sem=ici_send.at[side, i],
            recv_sem=ici_recv.at[side, i],
            device_id=(above if side == 0 else below, c),
            device_id_type=MESH,
        )

    def forward(side, i):
        return pltpu.make_async_remote_copy(
            src_ref=hbuf.at[side, 0, pl.ds(i * PIECE, PIECE), :],
            dst_ref=hbuf.at[side, 1, pl.ds(i * PIECE, PIECE), :],
            send_sem=fwd_send.at[side, i],
            recv_sem=fwd_recv.at[side, i],
            device_id=(lat, other),
            device_id_type=MESH,
        )

    for i in range(pieces):

        @pl.when(has_high)
        def _():
            crossing(0, i).start()

        @pl.when(has_low)
        def _():
            crossing(1, i).start()

    pairs = tiles // 2
    given = [
        (wq_in, wq2),
        (wk_in, wk2),
        (bias_in, bias2),
        (wv_in, wv2),
        (wo_in, wo2),
        (gain_in, gain2),
    ]
    gifts = [
        pltpu.make_async_remote_copy(
            src_ref=source,
            dst_ref=target,
            send_sem=w_send.at[i],
            recv_sem=w_recv.at[i],
            device_id=(lat, other),
            device_id_type=MESH,
        )
        for i, (source, target) in enumerate(given)
    ]
    for gift in gifts:
        gift.start()
    mine = [
        (mesh_in.at[pl.ds(pl.multiple_of(c * half, half), half), :], mesh_ref),
        (wq_in, wq_ref),
        (wk_in, wk_ref),
        (nb_in, nb_ref),
        (bias_in, bias_ref),
        (wv_in, wv_ref),
        (wo_in, wo_ref),
        (gain_in, gain_ref),
    ]
    mine = [pltpu.make_async_copy(source, target, local_sem.at[i]) for i, (source, target) in enumerate(mine)]
    for load in mine + loads:
        load.start()
    for load in mine:
        load.wait()

    mesh_rows = mesh_ref[...]

    def absorbed(part, wq, wk):
        q = jnp.dot(mesh_rows, wq[...], preferred_element_type=F32).astype(BF16)
        for j in range(2):
            s = slice(j * HEAD_DIM, (j + 1) * HEAD_DIM)
            qk = lax.dot_general(q[:, s], wk[:, s], NT, preferred_element_type=F32)
            qs[2 * part + j] = (qk * HEAD_DIM ** -0.5).astype(BF16)

    flat = table.reshape(table.shape[0] * 4, 128)

    def convert(rows, at, count):
        for col in range(4):
            flat[pl.ds(at * 4 + col, count, stride=4), :] = rows[:, col * 128:(col + 1) * 128].astype(F32)

    absorbed(0, wq_ref, wk_ref)
    for i in range(chunks):
        loads[i].wait()
        convert(buf.at[pl.ds(i * CH, CH), :], HALO + i * CH, CH)
    for gift in gifts:
        gift.wait()
    absorbed(1, wq2, wk2)

    node = lax.broadcasted_iota(jnp.int32, (TN, EDGES), 0)
    lane = lax.broadcasted_iota(jnp.int32, (TN, EDGES), 1)
    same = (lane % TN) == node

    nb = nb_ref[...]
    local = nb - (lat * band - HALO)
    live = nb >= 0
    at_end = (local < HALO) | (local >= HALO + band)
    row = jnp.where(live, jnp.where(at_end, local ^ (c * share), local), HALO)
    row = jnp.clip(row, 0, band + 2 * HALO - 1)
    stack = []
    for values in (bias_ref[...].astype(F32), bias2[...].astype(F32)):
        stack += [jnp.where(live, values[j * K:(j + 1) * K, :], DEAD) for j in range(2)]
    stack += [(row >> 6).astype(F32), (row & 63).astype(F32)]
    channels[...] = jnp.concatenate(stack, axis=0).T
    slot = lax.broadcasted_iota(jnp.int32, (K, EDGES), 0)
    slot_lane = lax.broadcasted_iota(jnp.int32, (K, EDGES), 1)
    place = jnp.where(slot_lane // TN == slot, 1.0, 0.0).astype(BF16)

    @pl.loop(0, pairs)
    def _(i):
        lines = []
        for j in range(2):
            r0 = pl.multiple_of(c * half + (2 * i + j) * TN, TN)
            mixed = channels[pl.ds(r0, TN), :]
            parts = jnp.concatenate([mixed[:, n * K:(n + 1) * K] for n in range(6)], axis=0).astype(BF16)
            wide = jnp.dot(parts, place, preferred_element_type=F32)
            line = [
                jnp.sum(jnp.where(same, wide[n * TN:(n + 1) * TN], 0.0), axis=0, keepdims=True) for n in range(6)
            ]
            rows_v[2 * i + j] = jnp.clip((line[4] * 64.0 + line[5]).astype(jnp.int32), 0, band + 2 * HALO - 1) * 4
            lines.append(line)
        spread[i] = jnp.concatenate(lines[0][0:2] + lines[1][0:2] + lines[0][2:4] + lines[1][2:4], axis=0)

    fetches = [pltpu.make_async_copy(rows_v.at[t], row_refs[t], s_sem.at[t]) for t in range(tiles)]
    for fetch in fetches:
        fetch.start()

    side_rows = (0, HALO + band)

    def arrive(side, i):
        crossing(side, i).wait_recv()
        forward(side, i).start()

    def arrived(side, i):
        convert(hbuf.at[side, 0, pl.ds(i * PIECE, PIECE), :], side_rows[side] + i * PIECE, PIECE)

    def arrive_forwarded(side, i):
        forward(side, i).wait()
        convert(hbuf.at[side, 1, pl.ds(i * PIECE, PIECE), :], side_rows[side] + share + i * PIECE, PIECE)

    for i in range(pieces + 1):
        for side, has in ((0, has_low), (1, has_high)):
            if i < pieces:
                pl.when(has)(functools.partial(arrive, side, i))
        for side, has in ((0, has_low), (1, has_high)):
            if i < pieces:
                pl.when(has)(functools.partial(arrived, side, i))
        for side, has in ((0, has_low), (1, has_high)):
            if i > 0:
                pl.when(has)(functools.partial(arrive_forwarded, side, i - 1))

    for fetch in fetches:
        fetch.wait()

    def gather(t, st):
        for p in range(EDGES):
            st[p] = flat[pl.ds(row_refs[t][0, p], 4), :]

    def scores(t, st):
        st = st.reshape(EDGES * 4, 128)
        g = jnp.concatenate([st[pl.ds(col, EDGES, stride=4), :].astype(BF16) for col in range(4)], axis=1)
        gs[t * EDGES:(t + 1) * EDGES, :] = g
        qt = jnp.concatenate([qs[h, t * TN:(t + 1) * TN, :] for h in range(HEADS)], axis=0)
        sc = lax.dot_general(qt, g, NT, preferred_element_type=F32)
        return [jnp.sum(jnp.where(same, sc[h * TN:(h + 1) * TN], 0.0), axis=0, keepdims=True) for h in range(HEADS)]

    stages = (st0, st1)
    gather(0, st0)
    lines = []
    for t in range(tiles):
        if t + 1 < tiles:
            gather(t + 1, stages[(t + 1) % 2])
        lines.append(scores(t, stages[t % 2]))
        if t % 2:
            s0, s1 = lines[t - 1], lines[t]
            ss[t // 2] = jnp.concatenate(s0[0:2] + s1[0:2] + s0[2:4] + s1[2:4], axis=0)

    blocks = EDGES // 128

    def fold(x, op):
        y = x[..., 0:128]
        for j in range(1, blocks):
            y = op(y, x[..., j * 128:(j + 1) * 128])
        y = op(y, pltpu.roll(y, 64, y.ndim - 1))
        return op(y, pltpu.roll(y, 32, y.ndim - 1))

    s = ss[...] + spread[...]
    m = fold(s, jnp.maximum)
    w = jnp.exp(s - jnp.concatenate([m] * blocks, axis=2))
    total = fold(w, jnp.add)
    ss[...] = w * jnp.concatenate([1.0 / total] * blocks, axis=2)

    for i in range(pairs):
        both = ss[i]
        for j in range(2):
            t = 2 * i + j
            rows = [both[part * 4 + j * 2 + h:part * 4 + j * 2 + h + 1] for part in range(2) for h in range(2)]
            pt = jnp.concatenate([jnp.where(same, row, 0.0).astype(BF16) for row in rows], axis=0)
            g = gs[t * EDGES:(t + 1) * EDGES, :]
            ctx = jnp.dot(pt, g, preferred_element_type=F32)
            for h in range(HEADS):
                cs[h, t * TN:(t + 1) * TN, :] = ctx[h * TN:(h + 1) * TN].astype(BF16)

    projected = jnp.zeros((half, D), F32)
    for part, (wv, wo) in enumerate(((wv_ref, wo_ref), (wv2, wo2))):
        attended = [
            jnp.dot(cs[2 * part + j], wv[:, j * HEAD_DIM:(j + 1) * HEAD_DIM], preferred_element_type=F32).astype(BF16)
            for j in range(2)
        ]
        projected = projected + jnp.dot(jnp.concatenate(attended, axis=1), wo[...], preferred_element_type=F32)
    updated = mesh_ref[...].astype(F32) + projected
    mean = jnp.sum(updated, axis=1, keepdims=True) / D
    variance = jnp.sum(updated * updated, axis=1, keepdims=True) / D - mean * mean
    normed = (updated - mean) * lax.rsqrt(variance + EPSILON)
    left, right = normed[:, 0:D // 2], normed[:, D // 2:D]
    first = c == 0
    gains = [gain_ref[...].astype(F32).reshape(1, D // 2), gain2[...].astype(F32).reshape(1, D // 2)]
    out_send[...] = (jnp.where(first, right, left) * gains[1]).astype(BF16)
    out_keep[...] = (jnp.where(first, left, right) * gains[0]).astype(BF16)
    out_rows = out_ref.at[pl.ds(pl.multiple_of(c * half, half), half), :]
    swap = pltpu.make_async_remote_copy(
        src_ref=out_send,
        dst_ref=out_rows,
        send_sem=x_send,
        recv_sem=x_recv,
        device_id=(lat, other),
        device_id_type=MESH,
    )
    swap.start()
    keep = pltpu.make_async_copy(out_keep, out_rows, local_sem.at[0])
    keep.start()
    keep.wait()
    swap.wait()
    for side, has in ((0, has_high), (1, has_low)):
        for i in range(pieces):

            @pl.when(has)
            def _():
                crossing(side, i).wait_send()


def shards(
    grid_latent, mesh_latent, neighbours, edge_bias, query_weight, key_weight, value_weight, out_weight, norm_gain
):
    band = grid_latent.shape[0]
    count = mesh_latent.shape[0]
    half = count // 2
    tiles = half // TN
    pieces = HALO // 2 // PIECE
    width = D // 2
    dma = pltpu.SemaphoreType.DMA
    out = pl.pallas_call(
        functools.partial(kernel, lax.axis_size("lat") - 1),
        out_shape=jax.ShapeDtypeStruct((count, width), BF16),
        in_specs=[ANY] * 9,
        out_specs=ANY,
        scratch_shapes=[
            pltpu.VMEM((band, D), BF16),
            pltpu.VMEM((2, 2, HALO // 2, D), BF16),
            pltpu.VMEM((band + 2 * HALO, 4, 128), F32),
            pltpu.VMEM((EDGES, 4, 128), F32),
            pltpu.VMEM((EDGES, 4, 128), F32),
            pltpu.VMEM((HEADS, half, D), BF16),
            pltpu.VMEM((HEADS, half, D), BF16),
            pltpu.VMEM((tiles * EDGES, D), BF16),
            pltpu.VMEM((tiles // 2, 8, EDGES), F32),
            pltpu.VMEM((D, width), BF16),
            pltpu.VMEM((D, width), BF16),
            pltpu.VMEM((D, width), BF16),
            pltpu.VMEM((width, D), BF16),
            pltpu.VMEM((width,), BF16),
            pltpu.VMEM((2 * K, count), BF16),
            pltpu.VMEM((half, width), BF16),
            pltpu.VMEM((half, width), BF16),
            pltpu.VMEM((K, count), jnp.int32),
            pltpu.VMEM((2 * K, count), BF16),
            pltpu.VMEM((half, D), BF16),
            pltpu.VMEM((D, width), BF16),
            pltpu.VMEM((D, width), BF16),
            pltpu.VMEM((D, width), BF16),
            pltpu.VMEM((width, D), BF16),
            pltpu.VMEM((width,), BF16),
            dma((8,)),
            pltpu.VMEM((count, 6 * K), F32),
            pltpu.VMEM((tiles // 2, 8, EDGES), F32),
            pltpu.VMEM((tiles, 1, EDGES), jnp.int32),
            dma((band // CH,)),
            dma((2, pieces)),
            dma((2, pieces)),
            dma((2, pieces)),
            dma((2, pieces)),
            dma((6,)),
            dma((6,)),
            dma,
            dma,
            dma((tiles,)),
        ]
        + [pltpu.SMEM((1, EDGES), jnp.int32)] * tiles,
        compiler_params=pltpu.CompilerParams(
            collective_id=0, has_side_effects=True, vmem_limit_bytes=60 * 1024 * 1024
        ),
    )(
        grid_latent, neighbours.T, edge_bias.T, mesh_latent, query_weight, key_weight, value_weight, out_weight,
        norm_gain,
    )
    return out


def solution(mesh):
    in_specs = (
        P("lat", None),
        P("lat", None),
        P("lat", None),
        P("lat", "head"),
        P(None, "head"),
        P(None, "head"),
        P(None, "head"),
        P("head", None),
        P("head"),
    )
    out_specs = P("lat", "head")
    return jax.shard_map(shards, mesh=mesh, in_specs=in_specs, out_specs=out_specs, check_vma=False)
```
